32 devices in a mesh: sample: 8 (over y, x, core), line: 4 (over z).
Axes of the slice: x: 2, y: 2, z: 4, core: 2. Of those that a mesh axis runs over, the one named last changes fastest.
Arguments:
- wind_dev: bfloat16 [4096, 10000], P('sample', 'line'), may hold values from -6 to 6
- ptdf: bfloat16 [4096, 10000], P('line'), may hold values from -0.0625 to 0.0625
- region_weights: bfloat16 [31, 10000], replicated, may hold values from -0.0625 to 0.0625
- incidence: int32 [12706, 2], replicated, may hold values from 0 to 9999
- monitored: int32 [4096], P('line'), may hold values from 0 to 12705
- ratings: float32 [12706], replicated, may hold values from 1 to 3
- base_flow: float32 [4096], P('line'), may hold values from -6 to 6
- line_cost: float32 [4096], P('line'), may hold values from 0.2 to 20
- policy: float32 [32, 4096], P(None, 'line'), may hold values from -0.6 to 0.6
Outputs:
- new_policy: float32 [32, 4096], P(None, 'line')
- new_flows: float32 [4096, 4096], P('sample', 'line')
- decrement: float32 [], replicated
- grad_norm: float32 [], replicated
The draws below stay inside these ranges and needn't reach their ends.
All inputs are finite; a program needn't handle non-finite values.
Results may differ from the reference program's by a relative error of at most 0.0003.
Values may be sent and summed in bfloat16 or wider, within the bound.
A program may use at most 128 MiB of HBM per device.

```python
import math
import jax
import jax.numpy as jnp
from jax import lax

NUM_BUSES = 10000
MONITORED = 4096
GRID_LINES = 12706
REGIONS = 31
FEATURES = 32
SCENARIOS = 4096


def draw_line_cost(key, part):
    position = jnp.arange(MONITORED, dtype=jnp.float32) / MONITORED
    low_end = 0.3
    high_end = 3.0
    rise_rate = 1.1
    uniform_draw = jax.random.uniform(key, (MONITORED,), jnp.float32)
    spread_term = jnp.exp(jnp.log(low_end) + uniform_draw * (jnp.log(high_end) - jnp.log(low_end)))
    return spread_term * jnp.exp(rise_rate * position)


def with_ends(drawn, rng, low, high):
    longest = drawn.shape.index(max(drawn.shape))
    spots = []
    for shift in (0, 1):
        where = [jax.random.randint(jax.random.fold_in(rng, axis), (), 0, length) for axis, length in enumerate(drawn.shape)]
        where[longest] = (where[longest] + shift) % drawn.shape[longest]
        spots.append(tuple(where))
    return drawn.at[spots[0]].set(low).at[spots[1]].set(high)


def steps_of(own_key, extent, cuts, low, largest):
    loudness, own = 1.0, jax.random.fold_in(own_key, 6)
    for dim, parts in cuts:
        steps = jnp.exp(jax.random.uniform(jax.random.fold_in(own, dim), (parts,), jnp.float32, low / len(cuts), largest / len(cuts)))
        loudness = loudness * jnp.repeat(steps, extent[dim] // parts).reshape([-1 if axis == dim else 1 for axis in range(len(extent))])
    return loudness


def noise(stream_key, dims, scale, reach, shards=(), held_as=jnp.bfloat16):
    result = jax.random.normal(stream_key, dims, jnp.float32) * scale
    if len(shards) > 0:
        result = steps_of(stream_key, dims, shards, -0.22, 0.18) * result
    return jnp.clip(result, min=-reach, max=reach).astype(held_as)


def setup_inputs(seed: int = 0) -> dict:
    key_of = jax.random.split(jax.random.key(seed), 10)
    return {
        "wind_dev": noise(key_of[0], (SCENARIOS, NUM_BUSES), 1.0, 6.0, ((0, 8), (1, 4))),
        "ptdf": noise(key_of[1], (MONITORED, NUM_BUSES), NUM_BUSES ** -0.5, 0.0625, ((0, 4),)),
        "region_weights": noise(key_of[2], (REGIONS, NUM_BUSES), NUM_BUSES ** -0.5, 0.0625),
        "incidence": with_ends(jax.random.randint(key_of[3], (GRID_LINES, 2), 0, NUM_BUSES), jax.random.fold_in(key_of[3], 1), 0, NUM_BUSES - 1).astype(jnp.int32),
        "monitored": with_ends(jax.random.randint(key_of[4], (MONITORED,), 0, GRID_LINES), jax.random.fold_in(key_of[4], 1), 0, GRID_LINES - 1).astype(jnp.int32),
        "ratings": jnp.clip(jnp.exp(jax.random.uniform(key_of[5], (GRID_LINES,), jnp.float32, math.log(1.0), math.log(3.0))), 1.0, 3.0),
        "base_flow": noise(key_of[6], (MONITORED,), 1.0, 6.0, ((0, 4),), jnp.float32),
        "line_cost": draw_line_cost(jax.random.fold_in(key_of[9], 71), 0),
        "policy": jnp.clip(jax.random.uniform(key_of[8], (FEATURES, MONITORED), jnp.float32, -0.6, 0.6) * steps_of(key_of[8], (FEATURES, MONITORED), ((1, 4),), -0.4, 0.0), -0.6, 0.6),
    }


ridge_weight = 1.0
barrier_weight = 0.1
smoothing = 0.5

def penalty_terms(factors, ends_diff, slope_term, curve_term, weight):
    highest = lax.Precision.HIGHEST
    regions = factors.shape[1]
    lines_here = slope_term.shape[1]
    outer_prod = (factors[:, :, None] * factors[:, None, :]).reshape(factors.shape[0], regions * regions)
    block_rr = lax.dot_general(outer_prod, curve_term, (((0,), (0,)), ((), ())), precision=highest)
    weighted = curve_term * ends_diff
    cross_re = lax.dot_general(factors, weighted, (((0,), (0,)), ((), ())), precision=highest)
    corner = lax.optimization_barrier(jnp.sum(weighted * ends_diff, axis=0))
    upper_rows = jnp.concatenate([block_rr.reshape(regions, regions, lines_here), cross_re[:, None, :]], axis=1)
    bottom = jnp.concatenate([cross_re[None, :, :], corner[None, None, :]], axis=1)
    hessian = jnp.concatenate([upper_rows, bottom], axis=0) * weight
    grad_rr = lax.dot_general(factors, slope_term, (((0,), (0,)), ((), ())), precision=highest)
    gradient = jnp.concatenate([grad_rr, lax.optimization_barrier(jnp.sum(slope_term * ends_diff, axis=0))[None, :]], axis=0) * weight
    return (hessian.reshape((regions + 1) * (regions + 1), lines_here), gradient)

def factor_solve(hessian, gradient):
    features = gradient.shape[0]
    positions = jnp.arange(features, dtype=jnp.int32)

    def chol_column(column, lower_tri):
        target = lax.dynamic_index_in_dim(hessian, column, 1, keepdims=False)
        row_here = lax.dynamic_index_in_dim(lower_tri, column, 0, keepdims=False)
        running = target - lax.optimization_barrier(jnp.sum(lower_tri * row_here[None, :, :], axis=1))
        pivot_val = jnp.sqrt(lax.dynamic_index_in_dim(running, column, 0, keepdims=False))
        new_col = jnp.where((positions >= column)[:, None], running / pivot_val[None, :], jnp.zeros_like(running))
        select = (positions == column).astype(hessian.dtype)
        return lower_tri + new_col[:, None, :] * select[None, :, None]
    lower_tri = lax.fori_loop(0, features, chol_column, jnp.zeros_like(hessian))

    def forward_row(row_index, forward):
        row_here = lax.dynamic_index_in_dim(lower_tri, row_index, 0, keepdims=False)
        running = lax.dynamic_index_in_dim(gradient, row_index, 0, keepdims=False) - lax.optimization_barrier(jnp.sum(row_here * forward, axis=0))
        value = running / lax.dynamic_index_in_dim(row_here, row_index, 0, keepdims=False)
        select = (positions == row_index).astype(gradient.dtype)
        return forward + select[:, None] * value[None, :]
    forward = lax.fori_loop(0, features, forward_row, jnp.zeros_like(gradient))

    def backward_row(turn, backward):
        row_index = features - 1 - turn
        col_here = lax.dynamic_index_in_dim(lower_tri, row_index, 1, keepdims=False)
        running = lax.dynamic_index_in_dim(forward, row_index, 0, keepdims=False) - lax.optimization_barrier(jnp.sum(col_here * backward, axis=0))
        value = running / lax.dynamic_index_in_dim(col_here, row_index, 0, keepdims=False)
        select = (positions == row_index).astype(gradient.dtype)
        return backward + select[:, None] * value[None, :]
    backward = lax.fori_loop(0, features, backward_row, jnp.zeros_like(gradient))
    return (forward, -backward)

def owner_step(hessian_flat, gradient, policy_part):
    features = gradient.shape[0]
    lines_here = gradient.shape[1]
    hessian = hessian_flat.reshape(features, features, lines_here)
    margin_sq = 1.0 - policy_part * policy_part
    diag_terms = ridge_weight + barrier_weight * 2.0 * (1.0 + policy_part * policy_part) / (margin_sq * margin_sq)
    hessian = hessian + jnp.eye(features, dtype=hessian.dtype)[:, :, None] * diag_terms[:, None, :]
    gradient = gradient + ridge_weight * policy_part + barrier_weight * 2.0 * policy_part / margin_sq
    forward, newton_step = factor_solve(hessian, gradient)
    return (gradient, forward, newton_step)

def reference(wind_dev, ptdf, region_weights, incidence, monitored, ratings, base_flow, line_cost, policy):
    highest = lax.Precision.HIGHEST
    regions = region_weights.shape[0]
    endpoints = jnp.take(incidence, monitored, axis=0)
    from_bus = endpoints[:, 0]
    to_bus = endpoints[:, 1]
    rating = jnp.take(ratings, monitored)
    total_scen = wind_dev.shape[0]
    grid_flow = jnp.dot(wind_dev, ptdf.T, preferred_element_type=jnp.float32)
    factors = jnp.dot(wind_dev, region_weights.T, preferred_element_type=jnp.float32)
    ends_diff = jnp.take(wind_dev, to_bus, axis=1).astype(jnp.float32) - jnp.take(wind_dev, from_bus, axis=1).astype(jnp.float32)
    line_flow = grid_flow + base_flow[None, :] + jnp.dot(factors, policy[:regions], precision=highest) + policy[regions][None, :] * ends_diff
    prob_up = jax.nn.sigmoid((line_flow - rating[None, :]) / smoothing)
    prob_down = jax.nn.sigmoid((-line_flow - rating[None, :]) / smoothing)
    slope_term = prob_up - prob_down
    curve_term = (prob_up * (1.0 - prob_up) + prob_down * (1.0 - prob_down)) / smoothing
    weight = line_cost / total_scen
    hessian_sum, gradient_sum = penalty_terms(factors, ends_diff, slope_term, curve_term, weight)
    gradient, forward, newton_step = owner_step(hessian_sum, gradient_sum, policy)
    decrement_sq = jnp.sum(forward * forward)
    norm_sq = jnp.sum(gradient * gradient)
    features = policy.shape[0]
    step_length = 1.0 / (1.0 + jnp.sqrt(decrement_sq / (barrier_weight * features * MONITORED)))
    new_policy = policy + step_length * newton_step
    shift_flow = jnp.dot(factors, newton_step[:regions], precision=highest) + newton_step[regions][None, :] * ends_diff
    new_flows = line_flow + step_length * shift_flow
    return (new_policy, new_flows, jnp.sqrt(decrement_sq), jnp.sqrt(norm_sq))
```

```python
import jax
import jax.numpy as jnp
from jax import lax
from jax.experimental import pallas as pl
from jax.experimental.pallas import tpu as pltpu
from jax.sharding import PartitionSpec as P

ridge_weight = 1.0
barrier_weight = 0.1
smoothing = 0.5


HIGH = lax.Precision.HIGH


def solve_lines(regions, packed_ref, weight_ref, policy_ref, out_ref, cols_ref):
    features = regions + 1
    weight = weight_ref[...]
    policy = policy_ref[...]
    margin_sq = 1.0 - policy * policy
    diag_terms = ridge_weight + barrier_weight * 2.0 * (1.0 + policy * policy) / (
        margin_sq * margin_sq
    )
    cols_ref[...] = jnp.zeros_like(cols_ref)
    bands = (regions + 1) // 2
    for band in range(bands):
        rows = packed_ref[band * features : (band + 1) * features, :] * weight
        if band == 0:
            rows = rows + diag_terms
        for i in range(regions):
            j = (i + band) % regions
            cols_ref[min(i, j), max(i, j) : max(i, j) + 1, :] = rows[i : i + 1]
    cross = packed_ref[bands * features : (bands + 1) * features, :] * weight
    for i in range(regions):
        cols_ref[i, regions : regions + 1, :] = cross[i : i + 1]
    cols_ref[regions, regions : regions + 1, :] = cross[regions:] + diag_terms[regions:]
    gradient = packed_ref[(bands + 1) * features : (bands + 2) * features, :] * weight
    gradient = gradient + ridge_weight * policy + barrier_weight * 2.0 * policy / margin_sq
    grad_sq = jnp.sum(gradient * gradient, axis=0, keepdims=True)

    positions = lax.broadcasted_iota(jnp.int32, gradient.shape, 0)
    inverses, forward = [], []
    running = gradient
    forward_sq = jnp.zeros_like(weight)
    for k in range(features):
        column = cols_ref[k]
        inverse = 1.0 / jnp.sqrt(column[k : k + 1])
        column = jnp.where(positions >= k, column * inverse, 0.0)
        cols_ref[k] = column
        value = running[k : k + 1] * inverse
        running = running - column * value
        forward_sq = forward_sq + value * value
        inverses.append(inverse)
        forward.append(value)
        for j in range(k + 1, features):
            base = j // 8 * 8
            cols_ref[j, base:, :] = cols_ref[j, base:, :] - column[base:] * column[j : j + 1]
    solved = jnp.zeros_like(gradient)
    for k in reversed(range(features)):
        value = (
            forward[k] - jnp.sum(cols_ref[k] * solved, axis=0, keepdims=True)
        ) * inverses[k]
        solved = jnp.where(positions == k, value, solved)
    out_ref[...] = jnp.zeros_like(out_ref)
    out_ref[:features, :] = -solved
    out_ref[features : features + 1, :] = forward_sq
    out_ref[features + 1 : features + 2, :] = grad_sq


def greet(partners):
    barrier = pltpu.get_barrier_semaphore()
    for partner in partners:
        pl.semaphore_signal(
            barrier, inc=1, device_id=partner, device_id_type=pl.DeviceIdType.MESH
        )
    pl.semaphore_wait(barrier, len(partners))


def sum_shares(samples, parts_ref, out_ref, near_ref, sums_ref, far_ref, sends, recvs):
    me = lax.axis_index("sample")
    pairs = samples // 2
    mine, side = me // 2, lax.rem(me, 2)
    others = [lax.rem(mine + i, pairs) for i in range(1, pairs)]
    partner = 2 * mine + (1 - side)
    greet([{"sample": partner}] + [{"sample": 2 * pair + side} for pair in others])
    near = []
    for slot, pair in enumerate(others + [mine]):
        near.append(
            pltpu.make_async_remote_copy(
                src_ref=parts_ref.at[2 * pair + (1 - side)],
                dst_ref=near_ref.at[slot],
                send_sem=sends.at[slot],
                recv_sem=recvs.at[slot],
                device_id={"sample": partner},
                device_id_type=pl.DeviceIdType.MESH,
            )
        )
        near[-1].start()
    for slot, pair in enumerate(others + [mine]):
        near[slot].wait_recv()
        sums_ref[slot] = parts_ref[2 * pair + side] + near_ref[slot]
    far = []
    for slot, pair in enumerate(others):
        far.append(
            pltpu.make_async_remote_copy(
                src_ref=sums_ref.at[slot],
                dst_ref=far_ref.at[slot],
                send_sem=sends.at[pairs + slot],
                recv_sem=recvs.at[pairs + slot],
                device_id={"sample": 2 * pair + side},
                device_id_type=pl.DeviceIdType.MESH,
            )
        )
        far[-1].start()
    out_ref[...] = sums_ref[pairs - 1]
    for slot in range(pairs - 1):
        far[slot].wait_recv()
        out_ref[...] += far_ref[slot]
    for copy in near + far:
        copy.wait_send()


def scatter_sum(parts):
    samples, rows, share = parts.shape
    pairs = samples // 2
    return pl.pallas_call(
        lambda *refs: sum_shares(samples, *refs),
        out_shape=jax.ShapeDtypeStruct((rows, share), parts.dtype),
        in_specs=[pl.BlockSpec(memory_space=pltpu.VMEM)],
        out_specs=pl.BlockSpec(memory_space=pltpu.VMEM),
        scratch_shapes=[
            pltpu.VMEM((pairs, rows, share), parts.dtype),
            pltpu.VMEM((pairs, rows, share), parts.dtype),
            pltpu.VMEM((pairs - 1, rows, share), parts.dtype),
            pltpu.SemaphoreType.DMA((2 * pairs - 1,)),
            pltpu.SemaphoreType.DMA((2 * pairs - 1,)),
        ],
        compiler_params=pltpu.CompilerParams(collective_id=0, has_side_effects=True),
        name="scatter_sum",
    )(parts)


def share_steps(samples, ring, features, solved_ref, all_ref, sums_ref, got_ref, mine_ref, far_ref, sends, recvs):
    me, place = lax.axis_index("sample"), lax.axis_index("line")
    peers = [lax.rem(me + i, samples) for i in range(1, samples)]
    lines = [lax.rem(place + i, ring) for i in range(1, ring)]
    greet([{"sample": peer} for peer in peers] + [{"line": line} for line in lines])
    copies = []
    for slot, peer in enumerate(peers):
        copies.append(
            pltpu.make_async_remote_copy(
                src_ref=solved_ref,
                dst_ref=got_ref.at[slot],
                send_sem=sends.at[slot],
                recv_sem=recvs.at[slot],
                device_id={"sample": peer},
                device_id_type=pl.DeviceIdType.MESH,
            )
        )
        copies[-1].start()
    total = solved_ref[features:, :]
    for slot in range(samples - 1):
        copies[slot].wait_recv()
        total = total + got_ref[slot, features:, :]
    mine_ref[...] = total
    all_ref[me] = solved_ref[:features, :]
    for slot in range(samples - 1):
        source = lax.rem(me + samples - 1 - slot, samples)
        all_ref[source] = got_ref[slot, :features, :]
    far = []
    for slot, line in enumerate(lines):
        far.append(
            pltpu.make_async_remote_copy(
                src_ref=mine_ref,
                dst_ref=far_ref.at[slot],
                send_sem=sends.at[samples - 1 + slot],
                recv_sem=recvs.at[samples - 1 + slot],
                device_id={"line": line},
                device_id_type=pl.DeviceIdType.MESH,
            )
        )
        far[-1].start()
    total = mine_ref[...]
    for slot in range(ring - 1):
        far[slot].wait_recv()
        total = total + far_ref[slot]
    sums_ref[...] = total
    for copy in copies + far:
        copy.wait_send()


def gather_steps(solved, features):
    samples, ring = lax.axis_size("sample"), lax.axis_size("line")
    rows, share = solved.shape
    vmem = pl.BlockSpec(memory_space=pltpu.VMEM)
    copies = samples + ring - 2
    return pl.pallas_call(
        lambda *refs: share_steps(samples, ring, features, *refs),
        out_shape=(
            jax.ShapeDtypeStruct((samples, features, share), solved.dtype),
            jax.ShapeDtypeStruct((rows - features, share), solved.dtype),
        ),
        in_specs=[vmem],
        out_specs=(vmem, vmem),
        scratch_shapes=[
            pltpu.VMEM((samples - 1, rows, share), solved.dtype),
            pltpu.VMEM((rows - features, share), solved.dtype),
            pltpu.VMEM((ring - 1, rows - features, share), solved.dtype),
            pltpu.SemaphoreType.DMA((copies,)),
            pltpu.SemaphoreType.DMA((copies,)),
        ],
        compiler_params=pltpu.CompilerParams(collective_id=1, has_side_effects=True),
        name="gather_steps",
    )(solved)


def split(value):
    top = value.astype(jnp.bfloat16)
    return top, (value - top.astype(jnp.float32)).astype(jnp.bfloat16)


def dot3(left, right):
    left_top, left_rest = split(left)
    right_top, right_rest = split(right)

    def product(a, b):
        return lax.dot_general(a, b, (((1,), (0,)), ((), ())), preferred_element_type=jnp.float32)

    return product(left_top, right_top) + (
        product(left_top, right_rest) + product(left_rest, right_top)
    )


def line_flows(
    samples, ring, chunk, block,
    wind_ref, ptdf_ref, weights_ref, ends_ref, base_ref, rating_ref, policy_ref,
    flow_ref, diff_ref, factors_ref, parts_ref,
    winds, grids, region_mix, stage, grid_sum, diff_sum, own_sem, stage_sems,
    send_up, recv_up, send_down, recv_down,
):
    me = lax.axis_index("line")
    regions = weights_ref.shape[0]
    features = regions + 1
    scen_here, width = wind_ref.shape
    lines_here = ptdf_ref.shape[0]
    share = lines_here // samples
    chunks = scen_here // chunk
    blocks = lines_here // block
    bands = (regions + 1) // 2
    reach = ring - 1
    barrier = pltpu.get_barrier_semaphore()

    @pl.when(me > 0)
    def _():
        pl.semaphore_signal(
            barrier, inc=1, device_id={"line": me - 1}, device_id_type=pl.DeviceIdType.MESH
        )

    @pl.when(me < ring - 1)
    def _():
        pl.semaphore_signal(
            barrier, inc=1, device_id={"line": me + 1}, device_id_type=pl.DeviceIdType.MESH
        )

    inner = jnp.logical_and(me > 0, me < ring - 1)

    @pl.when(inner)
    def _():
        pl.semaphore_wait(barrier, 2)

    @pl.when(jnp.logical_not(inner))
    def _():
        pl.semaphore_wait(barrier, 1)

    def rows_of(step):
        return pl.ds(step * chunk, chunk)

    def transfer(step, hops, side):
        piece = me - side * (hops - 1)
        slot = step * reach + hops - 1
        rows = rows_of(step)
        source = wind_ref.at[rows] if hops == 1 else winds.at[piece, rows]
        sends, recvs = (send_up, recv_up) if side == 1 else (send_down, recv_down)
        return pltpu.make_async_remote_copy(
            src_ref=source,
            dst_ref=winds.at[piece, rows],
            send_sem=sends.at[slot],
            recv_sem=recvs.at[slot],
            device_id={"line": me + side},
            device_id_type=pl.DeviceIdType.MESH,
        )

    def sends(hops, side):
        if side == 1:
            return jnp.logical_and(me >= hops - 1, me < ring - 1)
        return jnp.logical_and(me <= ring - hops, me > 0)

    def receives(hops, side):
        return me >= hops if side == 1 else me < ring - hops

    def launch(step, hops):
        for side in (1, -1):
            @pl.when(sends(hops, side))
            def _():
                transfer(step, hops, side).start()

    def arrival(step, hops, side):
        piece = me - side * hops
        slot = step * reach + hops - 1
        rows = rows_of(step)
        here = winds.at[piece, rows]
        recvs = recv_up if side == 1 else recv_down
        sends_ = send_up if side == 1 else send_down
        pltpu.make_async_remote_copy(
            src_ref=here,
            dst_ref=here,
            send_sem=sends_.at[slot],
            recv_sem=recvs.at[slot],
            device_id={"line": me - side},
            device_id_type=pl.DeviceIdType.MESH,
        ).wait_recv()

    launch(0, 1)
    if chunks > 1:
        launch(1, 1)
    own = pltpu.make_async_copy(wind_ref, winds.at[me], own_sem)
    own.start()

    def staged(index):
        slot = lax.rem(index, 2)
        return pltpu.make_async_copy(
            ptdf_ref.at[pl.ds(pl.multiple_of(index * block, block), block)],
            stage.at[slot],
            stage_sems.at[slot],
        )

    staged(0).start()
    region_mix[...] = jnp.zeros_like(region_mix)
    for piece in range(ring):
        region_mix[piece, :regions, :] = weights_ref[:, width * piece : width * (piece + 1)]

    def place(index, carry):
        @pl.when(index + 1 < blocks)
        def _():
            staged(index + 1).start()

        staged(index).wait()
        lines = pl.ds(pl.multiple_of(index * block, block), block)
        slot = lax.rem(index, 2)
        for piece in range(ring):
            grids[piece, lines, :] = stage[slot, :, width * piece : width * (piece + 1)]
        return carry

    lax.fori_loop(0, blocks, place, 0)
    own.wait()

    across = (((1,), (1,)), ((), ()))
    buses = lax.broadcasted_iota(jnp.int32, (block, width), 1)
    parts_ref[...] = jnp.zeros_like(parts_ref)

    def add_piece(step, piece, fresh):
        wind = winds[piece, rows_of(step), :]
        here = buses + piece * width

        def one(index, carry):
            lines = pl.ds(pl.multiple_of(index * block, block), block)
            pick = jnp.where(here == ends_ref[lines, 1:2], 1.0, 0.0) - jnp.where(
                here == ends_ref[lines, 0:1], 1.0, 0.0
            )
            grid = lax.dot_general(
                grids[piece, lines, :], wind, across, preferred_element_type=jnp.float32
            )
            diff = lax.dot_general(
                pick.astype(jnp.bfloat16), wind, across, preferred_element_type=jnp.float32
            )
            if fresh:
                grid_sum[lines, :] = grid
                diff_sum[lines, :] = diff
            else:
                grid_sum[lines, :] += grid
                diff_sum[lines, :] += diff
            return carry

        lax.fori_loop(0, blocks, one, 0)
        mix = lax.dot_general(
            region_mix[piece], wind, across, preferred_element_type=jnp.float32
        )
        where = rows_of(step)
        if fresh:
            factors_ref[:, where] = mix
        else:
            factors_ref[:, where] += mix

    def finish(step):
        where = rows_of(step)
        factors = factors_ref[:, where]
        doubled = jnp.concatenate(
            [factors[:regions], factors[:regions], factors[regions:]], axis=0
        )
        pairs = jnp.concatenate(
            [doubled[d : d + features] * factors for d in range(bands)], axis=0
        )
        turned = factors.T
        for index in range(blocks):
            lines = pl.ds(index * block, block)
            diff = diff_sum[lines, :].T
            flow = (
                grid_sum[lines, :].T
                + base_ref[:, lines]
                + dot3(turned, policy_ref[:, lines])
                + policy_ref[regions : regions + 1, lines] * diff
            )
            flow_ref[where, lines] = flow
            diff_ref[where, lines] = diff
            rating = rating_ref[:, lines]
            prob_up = jax.nn.sigmoid((flow - rating) / smoothing)
            prob_down = jax.nn.sigmoid((-flow - rating) / smoothing)
            slope = prob_up - prob_down
            curve = (prob_up * (1.0 - prob_up) + prob_down * (1.0 - prob_down)) / smoothing
            weighted = curve * diff
            block_sum = dot3(pairs, curve)
            cross = dot3(factors, weighted)
            tilt = dot3(factors, slope)
            corner = jnp.sum(weighted * diff, axis=0, keepdims=True)
            lift = jnp.sum(slope * diff, axis=0, keepdims=True)
            for inner in range(block // share):
                spot = index * (block // share) + inner
                cols = slice(inner * share, (inner + 1) * share)
                top = bands * features
                parts_ref[spot, :top, :] += block_sum[:, cols]
                parts_ref[spot, top : top + regions, :] += cross[:regions, cols]
                parts_ref[spot, top + regions : top + features, :] += corner[:, cols]
                low = top + features
                parts_ref[spot, low : low + regions, :] += tilt[:regions, cols]
                parts_ref[spot, low + regions : low + features, :] += lift[:, cols]

    for step in range(chunks):
        if step + 2 < chunks:
            launch(step + 2, 1)
        add_piece(step, me, True)
        for hops in range(1, ring):
            for side in (1, -1):
                @pl.when(receives(hops, side))
                def _():
                    arrival(step, hops, side)
            if hops < reach:
                launch(step, hops + 1)
            for side in (1, -1):
                @pl.when(receives(hops, side))
                def _():
                    add_piece(step, me - side * hops, False)
        finish(step)

    for step in range(chunks):
        for hops in range(1, ring):
            for side in (1, -1):
                @pl.when(sends(hops, side))
                def _():
                    transfer(step, hops, side).wait_send()


def flows_and_sums(wind_dev, ptdf, region_weights, endpoints, base_flow, rating, policy):
    samples, ring = lax.axis_size("sample"), lax.axis_size("line")
    scen_here, width = wind_dev.shape
    lines_here, total = ptdf.shape
    features = policy.shape[0]
    share = lines_here // samples
    chunk = 128
    block = max(128, lines_here // 4)
    while lines_here % block or block % share:
        block //= 2
    rows = ((features) // 2 + 2) * features
    copies = (scen_here // chunk) * (ring - 1)
    vmem = pl.BlockSpec(memory_space=pltpu.VMEM)
    anywhere = pl.BlockSpec(memory_space=pl.ANY)
    f32, bf16 = jnp.float32, jnp.bfloat16
    return pl.pallas_call(
        lambda *refs: line_flows(samples, ring, chunk, block, *refs),
        out_shape=(
            jax.ShapeDtypeStruct((scen_here, lines_here), f32),
            jax.ShapeDtypeStruct((scen_here, lines_here), f32),
            jax.ShapeDtypeStruct((features, scen_here), f32),
            jax.ShapeDtypeStruct((samples, rows, share), f32),
        ),
        in_specs=[anywhere, anywhere, vmem, vmem, vmem, vmem, vmem],
        out_specs=(vmem,) * 4,
        scratch_shapes=[
            pltpu.VMEM((ring, scen_here, width), bf16),
            pltpu.VMEM((ring, lines_here, width), bf16),
            pltpu.VMEM((ring, features, width), bf16),
            pltpu.VMEM((2, block, total), bf16),
            pltpu.VMEM((lines_here, chunk), f32),
            pltpu.VMEM((lines_here, chunk), f32),
            pltpu.SemaphoreType.DMA,
            pltpu.SemaphoreType.DMA((2,)),
            pltpu.SemaphoreType.DMA((copies,)),
            pltpu.SemaphoreType.DMA((copies,)),
            pltpu.SemaphoreType.DMA((copies,)),
            pltpu.SemaphoreType.DMA((copies,)),
        ],
        compiler_params=pltpu.CompilerParams(
            collective_id=2, has_side_effects=True, vmem_limit_bytes=66 * 1000 * 1000
        ),
        name="line_flows",
    )(wind_dev, ptdf, region_weights, endpoints, base_flow[None, :], rating[None, :], policy)


def shards(
    wind_dev, ptdf, region_weights, incidence, monitored, ratings, base_flow, line_cost, policy
):
    regions = region_weights.shape[0]
    features = regions + 1
    scen_here = wind_dev.shape[0]
    lines_here = ptdf.shape[0]
    ring = lax.axis_size("line")
    samples = lax.axis_size("sample")

    endpoints = jnp.take(incidence, monitored, axis=0)
    rating = jnp.take(ratings, monitored)
    line_flow, ends_diff, factors, parts = flows_and_sums(
        wind_dev, ptdf, region_weights, endpoints, base_flow, rating, policy
    )
    packed = scatter_sum(parts)
    share = packed.shape[1]
    start = lax.axis_index("sample") * share
    weight_share = lax.dynamic_slice_in_dim(line_cost, start, share)[None, :] / (
        scen_here * samples
    )
    policy_share = lax.dynamic_slice_in_dim(policy, start, share, 1)
    solved = pl.pallas_call(
        lambda *refs: solve_lines(regions, *refs),
        out_shape=jax.ShapeDtypeStruct((features + 8, share), jnp.float32),
        scratch_shapes=[pltpu.VMEM((features, features, share), jnp.float32)],
        name="solve_lines",
    )(packed, weight_share, policy_share)
    steps, sums = gather_steps(solved, features)
    full_step = steps.transpose(1, 0, 2).reshape(features, lines_here)
    decrement_sq, norm_sq = jnp.sum(sums[:2], axis=1)

    total_lines = lines_here * ring
    step_length = 1.0 / (1.0 + jnp.sqrt(decrement_sq / (barrier_weight * features * total_lines)))
    new_policy = policy + step_length * full_step
    over_first = (((0,), (0,)), ((), ()))
    shift_flow = (
        lax.dot_general(factors, full_step, over_first, precision=HIGH)
        + full_step[regions][None, :] * ends_diff
    )
    new_flows = line_flow + step_length * shift_flow
    return (new_policy, new_flows, jnp.sqrt(decrement_sq), jnp.sqrt(norm_sq))


def solution(mesh):
    placed = (
        P("sample", "line"),
        P("line", None),
        P(),
        P(),
        P("line"),
        P(),
        P("line"),
        P("line"),
        P(None, "line"),
    )
    return jax.shard_map(
        shards,
        mesh=mesh,
        in_specs=placed,
        out_specs=(P(None, "line"), P("sample", "line"), P(), P()),
        check_vma=False,
    )
```

```python
import jax
import jax.numpy as jnp
from jax import lax
from jax.experimental import pallas as pl
from jax.experimental.pallas import tpu as pltpu
from jax.sharding import PartitionSpec as P

ridge_weight = 1.0
barrier_weight = 0.1
smoothing = 0.5

HIGH = lax.Precision.HIGH


def solve_lines(regions, packed_ref, weight_ref, policy_ref, out_ref, cols_ref):
    features = regions + 1
    weight = weight_ref[...]
    policy = policy_ref[...]
    margin_sq = 1.0 - policy * policy
    diag_terms = ridge_weight + barrier_weight * 2.0 * (1.0 + policy * policy) / (
        margin_sq * margin_sq
    )
    cols_ref[...] = jnp.zeros_like(cols_ref)
    bands = (regions + 1) // 2
    for band in range(bands):
        rows = packed_ref[band * features : (band + 1) * features, :] * weight
        if band == 0:
            rows = rows + diag_terms
        for i in range(regions):
            j = (i + band) % regions
            cols_ref[min(i, j), max(i, j) : max(i, j) + 1, :] = rows[i : i + 1]
    cross = packed_ref[bands * features : (bands + 1) * features, :] * weight
    for i in range(regions):
        cols_ref[i, regions : regions + 1, :] = cross[i : i + 1]
    cols_ref[regions, regions : regions + 1, :] = cross[regions:] + diag_terms[regions:]
    gradient = packed_ref[(bands + 1) * features : (bands + 2) * features, :] * weight
    gradient = gradient + ridge_weight * policy + barrier_weight * 2.0 * policy / margin_sq
    grad_sq = jnp.sum(gradient * gradient, axis=0, keepdims=True)

    positions = lax.broadcasted_iota(jnp.int32, gradient.shape, 0)
    inverses, forward = [], []
    running = gradient
    forward_sq = jnp.zeros_like(weight)
    for k in range(features):
        column = cols_ref[k]
        inverse = 1.0 / jnp.sqrt(column[k : k + 1])
        column = jnp.where(positions >= k, column * inverse, 0.0)
        cols_ref[k] = column
        value = running[k : k + 1] * inverse
        running = running - column * value
        forward_sq = forward_sq + value * value
        inverses.append(inverse)
        forward.append(value)
        for j in range(k + 1, features):
            base = j // 8 * 8
            cols_ref[j, base:, :] = cols_ref[j, base:, :] - column[base:] * column[j : j + 1]
    solved = jnp.zeros_like(gradient)
    for k in reversed(range(features)):
        value = (
            forward[k] - jnp.sum(cols_ref[k] * solved, axis=0, keepdims=True)
        ) * inverses[k]
        solved = jnp.where(positions == k, value, solved)
    out_ref[...] = jnp.zeros_like(out_ref)
    out_ref[:features, :] = -solved
    out_ref[features : features + 1, :] = forward_sq
    out_ref[features + 1 : features + 2, :] = grad_sq


def greet(partners):
    barrier = pltpu.get_barrier_semaphore()
    for partner in partners:
        pl.semaphore_signal(
            barrier, inc=1, device_id=partner, device_id_type=pl.DeviceIdType.MESH
        )
    pl.semaphore_wait(barrier, len(partners))


def share_steps(samples, ring, features, solved_ref, all_ref, sums_ref, got_ref, mine_ref, far_ref, sends, recvs):
    me, place = lax.axis_index("sample"), lax.axis_index("line")
    peers = [lax.rem(me + i, samples) for i in range(1, samples)]
    lines = [lax.rem(place + i, ring) for i in range(1, ring)]
    copies = []
    for slot, peer in enumerate(peers):
        copies.append(
            pltpu.make_async_remote_copy(
                src_ref=solved_ref,
                dst_ref=got_ref.at[slot],
                send_sem=sends.at[slot],
                recv_sem=recvs.at[slot],
                device_id={"sample": peer},
                device_id_type=pl.DeviceIdType.MESH,
            )
        )
        copies[-1].start()
    total = solved_ref[features:, :]
    for slot in range(samples - 1):
        copies[slot].wait_recv()
        total = total + got_ref[slot, features:, :]
    mine_ref[...] = total
    all_ref[me] = solved_ref[:features, :]
    for slot in range(samples - 1):
        source = lax.rem(me + samples - 1 - slot, samples)
        all_ref[source] = got_ref[slot, :features, :]
    far = []
    for slot, line in enumerate(lines):
        far.append(
            pltpu.make_async_remote_copy(
                src_ref=mine_ref,
                dst_ref=far_ref.at[slot],
                send_sem=sends.at[samples - 1 + slot],
                recv_sem=recvs.at[samples - 1 + slot],
                device_id={"line": line},
                device_id_type=pl.DeviceIdType.MESH,
            )
        )
        far[-1].start()
    total = mine_ref[...]
    for slot in range(ring - 1):
        far[slot].wait_recv()
        total = total + far_ref[slot]
    sums_ref[...] = total
    for copy in copies + far:
        copy.wait_send()


def split(value):
    top = value.astype(jnp.bfloat16)
    return top, (value - top.astype(jnp.float32)).astype(jnp.bfloat16)


def dot3(left, right):
    left_top, left_rest = split(left)
    right_top, right_rest = split(right)

    def product(a, b):
        return lax.dot_general(a, b, (((1,), (0,)), ((), ())), preferred_element_type=jnp.float32)

    return product(left_top, right_top) + (
        product(left_top, right_rest) + product(left_rest, right_top)
    )


def split_rows(width, total, ring):
    rows = (width + 15 + 15) // 16 * 16
    starts = [min(piece * width // 16 * 16, total - rows) for piece in range(ring)]
    return rows, starts


def newton_kernel(
    samples, ring, chunk, block, group,
    wind_ref, ptdf_ref, weights_ref, ends_ref, ratings_ref, monitored_ref, base_ref, cost_ref,
    policy_ref,
    flow_ref, diff_ref, factors_ref, all_ref, sums_ref,
    winds, grids, region_mix, stage, table, found, spread, outbox, inbox, mix_inbox,
    packed, weight_mine, policy_mine, cols, solved, step_inbox, mine, far,
    own_sem, stage_sems, send_up, recv_up, send_down, recv_down,
    send_out, recv_out, send_mix, recv_mix, send_step, recv_step,
):
    me, mine_s = lax.axis_index("line"), lax.axis_index("sample")
    regions = weights_ref.shape[0]
    features = regions + 1
    width, scen_here = wind_ref.shape
    total, lines_here = ptdf_ref.shape
    grid_lines = ends_ref.shape[1]
    share = lines_here // samples
    chunks = scen_here // chunk
    blocks = lines_here // block
    bands = (regions + 1) // 2
    reach = ring - 1
    f32, bf16 = jnp.float32, jnp.bfloat16
    peers = [lax.rem(mine_s + i, samples) for i in range(1, samples)]
    greet(
        [{"line": lax.rem(me + i, ring)} for i in range(1, ring)]
        + [{"sample": peer} for peer in peers]
    )

    def rows_of(step):
        return pl.ds(step * chunk, chunk)

    def transfer(step, hops, side):
        piece = me - side * (hops - 1)
        slot = step * reach + hops - 1
        rows = rows_of(step)
        source = wind_ref.at[:, rows] if hops == 1 else winds.at[piece, :, rows]
        sends_, recvs = (send_up, recv_up) if side == 1 else (send_down, recv_down)
        return pltpu.make_async_remote_copy(
            src_ref=source,
            dst_ref=winds.at[piece, :, rows],
            send_sem=sends_.at[slot],
            recv_sem=recvs.at[slot],
            device_id={"line": me + side},
            device_id_type=pl.DeviceIdType.MESH,
        )

    def sends(hops, side):
        if side == 1:
            return jnp.logical_and(me >= hops - 1, me < ring - 1)
        return jnp.logical_and(me <= ring - hops, me > 0)

    def receives(hops, side):
        return me >= hops if side == 1 else me < ring - hops

    def launch(step, hops):
        for side in (1, -1):
            @pl.when(sends(hops, side))
            def _():
                transfer(step, hops, side).start()

    def arrival(step, hops, side):
        slot = step * reach + hops - 1
        here = winds.at[me - side * hops, :, rows_of(step)]
        pltpu.make_async_remote_copy(
            src_ref=here,
            dst_ref=here,
            send_sem=(send_up if side == 1 else send_down).at[slot],
            recv_sem=(recv_up if side == 1 else recv_down).at[slot],
            device_id={"line": me - side},
            device_id_type=pl.DeviceIdType.MESH,
        ).wait_recv()

    launch(0, 1)
    if chunks > 1:
        launch(1, 1)
    own = pltpu.make_async_copy(wind_ref, winds.at[me], own_sem)
    own.start()

    stage_rows, starts = split_rows(width, total, ring)

    def staged(piece, index):
        slot = lax.rem(index, 2)
        return pltpu.make_async_copy(
            ptdf_ref.at[
                pl.ds(starts[piece], stage_rows), pl.ds(pl.multiple_of(index * block, block), block)
            ],
            stage.at[slot],
            stage_sems.at[slot],
        )

    region_mix[...] = jnp.zeros_like(region_mix)
    for piece in range(ring):
        region_mix[piece, :regions, :] = weights_ref[:, width * piece : width * (piece + 1)]
        skip = width * piece - starts[piece]
        staged(piece, 0).start()

        def place(index, carry):
            @pl.when(index + 1 < blocks)
            def _():
                staged(piece, index + 1).start()

            staged(piece, index).wait()
            lines = pl.ds(pl.multiple_of(index * block, block), block)
            grids[piece, :, lines] = stage[lax.rem(index, 2), skip : skip + width, :]
            return carry

        lax.fori_loop(0, blocks, place, 0)

    ends = ends_ref[...]
    rating_all = ratings_ref[...]
    first = rating_all.astype(bf16).astype(f32)
    second = (rating_all - first).astype(bf16).astype(f32)
    third = rating_all - first - second
    table[...] = jnp.zeros_like(table)
    table[:, :grid_lines] = jnp.concatenate(
        [
            (ends // 256).astype(f32),
            lax.rem(ends, 256).astype(f32),
            first,
            second,
            third,
            jnp.zeros_like(first),
        ],
        axis=0,
    ).astype(bf16)
    found[...] = jnp.zeros_like(found)

    def lookup(index, carry):
        where = pl.ds(pl.multiple_of(index * group, group), group)
        hot = (
            lax.broadcasted_iota(jnp.int32, (group, lines_here), 0) + index * group
            == monitored_ref[...]
        )
        found[...] += lax.dot_general(
            table[:, where],
            jnp.where(hot, 1.0, 0.0).astype(bf16),
            (((1,), (0,)), ((), ())),
            preferred_element_type=f32,
        )
        return carry

    lax.fori_loop(0, table.shape[1] // group, lookup, 0)
    from_bus = found[0:1, :] * 256.0 + found[2:3, :]
    to_bus = found[1:2, :] * 256.0 + found[3:4, :]
    rating_row = found[4:5, :] + found[5:6, :] + found[6:7, :]
    found[0:1, :] = from_bus
    found[1:2, :] = to_bus
    for d in range(samples):
        cut = slice(d * share, (d + 1) * share)
        spread[d, :features, :] = policy_ref[:, cut]
        spread[d, features : features + 1, :] = cost_ref[:, cut]
        spread[d, features + 1 : features + 2, :] = rating_row[:, cut]
    policy_mine[...] = spread[mine_s, :features, :]
    weight_mine[...] = spread[mine_s, features : features + 1, :] / (scen_here * samples)
    packed[...] = jnp.zeros_like(packed)
    own.wait()

    forward = (((1,), (0,)), ((), ()))

    def add_piece(step, piece, fresh):
        rows = rows_of(step)
        wind = winds[piece, :, rows]
        turned = wind.T
        buses = (
            lax.broadcasted_iota(jnp.int32, (width, block), 0) + piece * width
        ).astype(f32)

        def one(index, carry):
            lines = pl.ds(pl.multiple_of(index * block, block), block)
            pick = jnp.where(buses == found[1:2, lines], 1.0, 0.0) - jnp.where(
                buses == found[0:1, lines], 1.0, 0.0
            )
            grid = lax.dot_general(
                turned, grids[piece, :, lines], forward, preferred_element_type=f32
            )
            diff = lax.dot_general(
                turned, pick.astype(bf16), forward, preferred_element_type=f32
            )
            if fresh:
                flow_ref[rows, lines] = grid
                diff_ref[rows, lines] = diff
            else:
                flow_ref[rows, lines] += grid
                diff_ref[rows, lines] += diff
            return carry

        lax.fori_loop(0, blocks, one, 0)
        mix = lax.dot_general(region_mix[piece], wind, forward, preferred_element_type=f32)
        if fresh:
            factors_ref[:, rows] = mix
        else:
            factors_ref[:, rows] += mix

    def finish(step):
        rows = rows_of(step)
        turned = factors_ref[:, rows].T
        mix_inbox[mine_s, step] = factors_ref[:, rows]
        diff = diff_ref[rows, :]
        flow = (
            flow_ref[rows, :]
            + base_ref[...]
            + dot3(turned, policy_ref[...])
            + policy_ref[regions:, :] * diff
        )
        flow_ref[rows, :] = flow
        for d in range(samples):
            cut = slice(d * share, (d + 1) * share)
            outbox[d, step, 0] = flow[:, cut]
            outbox[d, step, 1] = diff[:, cut]

    def parcel(step, slot, peer, source):
        spot = step * (samples - 1) + slot
        common = dict(device_id={"sample": peer}, device_id_type=pl.DeviceIdType.MESH)
        return (
            pltpu.make_async_remote_copy(
                src_ref=outbox.at[peer, step],
                dst_ref=inbox.at[source, step],
                send_sem=send_out.at[spot],
                recv_sem=recv_out.at[spot],
                **common,
            ),
            pltpu.make_async_remote_copy(
                src_ref=mix_inbox.at[mine_s, step],
                dst_ref=mix_inbox.at[source, step],
                send_sem=send_mix.at[spot],
                recv_sem=recv_mix.at[spot],
                **common,
            ),
        )

    def deliver(step):
        for slot, peer in enumerate(peers):
            for copy in parcel(step, slot, peer, mine_s):
                copy.start()

    def collect(step):
        inbox[mine_s, step] = outbox[mine_s, step]
        for slot in range(samples - 1):
            source = lax.rem(mine_s + samples - 1 - slot, samples)
            for copy in parcel(step, slot, source, source):
                copy.wait_recv()
        rating = spread[mine_s, features + 1 : features + 2, :]

        def one(source, carry):
            flow = inbox[source, step, 0]
            diff = inbox[source, step, 1]
            factors = mix_inbox[source, step]
            doubled = jnp.concatenate(
                [factors[:regions], factors[:regions], factors[regions:]], axis=0
            )
            pairs = jnp.concatenate(
                [doubled[d : d + features] * factors for d in range(bands)], axis=0
            )
            prob_up = jax.nn.sigmoid((flow - rating) / smoothing)
            prob_down = jax.nn.sigmoid((-flow - rating) / smoothing)
            slope = prob_up - prob_down
            curve = (prob_up * (1.0 - prob_up) + prob_down * (1.0 - prob_down)) / smoothing
            weighted = curve * diff
            top = bands * features
            packed[:top, :] += dot3(pairs, curve)
            packed[top : top + regions, :] += dot3(factors, weighted)[:regions]
            packed[top + regions : top + features, :] += jnp.sum(
                weighted * diff, axis=0, keepdims=True
            )
            low = top + features
            packed[low : low + regions, :] += dot3(factors, slope)[:regions]
            packed[low + regions : low + features, :] += jnp.sum(
                slope * diff, axis=0, keepdims=True
            )
            return carry

        lax.fori_loop(0, samples, one, 0)

    for step in range(chunks):
        if step + 2 < chunks:
            launch(step + 2, 1)
        add_piece(step, me, True)
        for hops in range(1, ring):
            for side in (1, -1):
                @pl.when(receives(hops, side))
                def _():
                    arrival(step, hops, side)
            if hops < reach:
                launch(step, hops + 1)
            for side in (1, -1):
                @pl.when(receives(hops, side))
                def _():
                    add_piece(step, me - side * hops, False)
        finish(step)
        deliver(step)
        if step > 0:
            collect(step - 1)
    collect(chunks - 1)
    solve_lines(regions, packed, weight_mine, policy_mine, solved, cols)
    share_steps(
        samples, ring, features, solved, all_ref, sums_ref, step_inbox, mine, far,
        send_step, recv_step,
    )
    for step in range(chunks):
        for hops in range(1, ring):
            for side in (1, -1):
                @pl.when(sends(hops, side))
                def _():
                    transfer(step, hops, side).wait_send()
        for slot, peer in enumerate(peers):
            for copy in parcel(step, slot, peer, mine_s):
                copy.wait_send()


def newton_steps(
    wind_dev, ptdf, region_weights, incidence, monitored, ratings, base_flow, line_cost, policy
):
    samples, ring = lax.axis_size("sample"), lax.axis_size("line")
    scen_here, width = wind_dev.shape
    lines_here, total = ptdf.shape
    features = policy.shape[0]
    share = lines_here // samples
    chunk = 128
    chunks = scen_here // chunk
    block = 256
    while lines_here % block:
        block //= 2
    group = 512
    table_cols = (incidence.shape[0] + group - 1) // group * group
    stage_rows, _ = split_rows(width, total, ring)
    packed_rows = (features // 2 + 2) * features
    hops = chunks * (ring - 1)
    parcels = chunks * (samples - 1)
    copies = samples + ring - 2
    vmem = pl.BlockSpec(memory_space=pltpu.VMEM)
    anywhere = pl.BlockSpec(memory_space=pl.ANY)
    f32, bf16 = jnp.float32, jnp.bfloat16
    dma = pltpu.SemaphoreType.DMA
    return pl.pallas_call(
        lambda *refs: newton_kernel(samples, ring, chunk, block, group, *refs),
        out_shape=(
            jax.ShapeDtypeStruct((scen_here, lines_here), f32),
            jax.ShapeDtypeStruct((scen_here, lines_here), f32),
            jax.ShapeDtypeStruct((features, scen_here), f32),
            jax.ShapeDtypeStruct((samples, features, share), f32),
            jax.ShapeDtypeStruct((8, share), f32),
        ),
        in_specs=[anywhere, anywhere] + [vmem] * 7,
        out_specs=(vmem,) * 5,
        scratch_shapes=[
            pltpu.VMEM((ring, width, scen_here), bf16),
            pltpu.VMEM((ring, width, lines_here), bf16),
            pltpu.VMEM((ring, features, width), bf16),
            pltpu.VMEM((2, stage_rows, block), bf16),
            pltpu.VMEM((8, table_cols), bf16),
            pltpu.VMEM((8, lines_here), f32),
            pltpu.VMEM((samples, features + 8, share), f32),
            pltpu.VMEM((samples, chunks, 2, chunk, share), f32),
            pltpu.VMEM((samples, chunks, 2, chunk, share), f32),
            pltpu.VMEM((samples, chunks, features, chunk), f32),
            pltpu.VMEM((packed_rows, share), f32),
            pltpu.VMEM((1, share), f32),
            pltpu.VMEM((features, share), f32),
            pltpu.VMEM((features, features, share), f32),
            pltpu.VMEM((features + 8, share), f32),
            pltpu.VMEM((samples - 1, features + 8, share), f32),
            pltpu.VMEM((8, share), f32),
            pltpu.VMEM((ring - 1, 8, share), f32),
            dma,
            dma((2,)),
            dma((hops,)),
            dma((hops,)),
            dma((hops,)),
            dma((hops,)),
            dma((parcels,)),
            dma((parcels,)),
            dma((parcels,)),
            dma((parcels,)),
            dma((copies,)),
            dma((copies,)),
        ],
        compiler_params=pltpu.CompilerParams(
            collective_id=0, has_side_effects=True, vmem_limit_bytes=67000000
        ),
        name="newton_steps",
    )(
        wind_dev.T, ptdf.T, region_weights, incidence.T, ratings[None, :], monitored[None, :],
        base_flow[None, :], line_cost[None, :], policy,
    )


def shards(
    wind_dev, ptdf, region_weights, incidence, monitored, ratings, base_flow, line_cost, policy
):
    features = policy.shape[0]
    regions = features - 1
    lines_here = ptdf.shape[0]
    ring = lax.axis_size("line")
    line_flow, ends_diff, factors, steps, sums = newton_steps(
        wind_dev, ptdf, region_weights, incidence, monitored, ratings, base_flow, line_cost, policy
    )
    full_step = steps.transpose(1, 0, 2).reshape(features, lines_here)
    decrement_sq, norm_sq = jnp.sum(sums[:2], axis=1)
    total_lines = lines_here * ring
    step_length = 1.0 / (1.0 + jnp.sqrt(decrement_sq / (barrier_weight * features * total_lines)))
    new_policy = policy + step_length * full_step
    over_first = (((0,), (0,)), ((), ()))
    shift_flow = (
        lax.dot_general(factors, full_step, over_first, precision=HIGH)
        + full_step[regions][None, :] * ends_diff
    )
    new_flows = line_flow + step_length * shift_flow
    return (new_policy, new_flows, jnp.sqrt(decrement_sq), jnp.sqrt(norm_sq))


def solution(mesh):
    placed = (
        P("sample", "line"),
        P("line", None),
        P(),
        P(),
        P("line"),
        P(),
        P("line"),
        P("line"),
        P(None, "line"),
    )
    return jax.shard_map(
        shards,
        mesh=mesh,
        in_specs=placed,
        out_specs=(P(None, "line"), P("sample", "line"), P(), P()),
        check_vma=False,
    )
```

```python
import jax
import jax.numpy as jnp
from jax import lax
from jax.experimental import pallas as pl
from jax.experimental.pallas import tpu as pltpu
from jax.sharding import PartitionSpec as P

ridge_weight = 1.0
barrier_weight = 0.1
smoothing = 0.5


def solve_lines(regions, packed_ref, weight_ref, policy_ref, out_ref, cols_ref):
    features = regions + 1
    weight = weight_ref[...]
    policy = policy_ref[...]
    margin_sq = 1.0 - policy * policy
    diag_terms = ridge_weight + barrier_weight * 2.0 * (1.0 + policy * policy) / (
        margin_sq * margin_sq
    )
    cols_ref[...] = jnp.zeros_like(cols_ref)
    bands = (regions + 1) // 2
    for band in range(bands):
        rows = packed_ref[band * features : (band + 1) * features, :] * weight
        if band == 0:
            rows = rows + diag_terms
        for i in range(regions):
            j = (i + band) % regions
            cols_ref[min(i, j), max(i, j) : max(i, j) + 1, :] = rows[i : i + 1]
    cross = packed_ref[bands * features : (bands + 1) * features, :] * weight
    for i in range(regions):
        cols_ref[i, regions : regions + 1, :] = cross[i : i + 1]
    cols_ref[regions, regions : regions + 1, :] = cross[regions:] + diag_terms[regions:]
    gradient = packed_ref[(bands + 1) * features : (bands + 2) * features, :] * weight
    gradient = gradient + ridge_weight * policy + barrier_weight * 2.0 * policy / margin_sq
    grad_sq = jnp.sum(gradient * gradient, axis=0, keepdims=True)

    positions = lax.broadcasted_iota(jnp.int32, gradient.shape, 0)
    inverses, forward = [], []
    running = gradient
    forward_sq = jnp.zeros_like(weight)
    for k in range(features):
        column = cols_ref[k]
        inverse = 1.0 / jnp.sqrt(column[k : k + 1])
        column = jnp.where(positions >= k, column * inverse, 0.0)
        cols_ref[k] = column
        value = running[k : k + 1] * inverse
        running = running - column * value
        forward_sq = forward_sq + value * value
        inverses.append(inverse)
        forward.append(value)
        for j in range(k + 1, features):
            base = j // 8 * 8
            cols_ref[j, base:, :] = cols_ref[j, base:, :] - column[base:] * column[j : j + 1]
    solved = jnp.zeros_like(gradient)
    for k in reversed(range(features)):
        value = (
            forward[k] - jnp.sum(cols_ref[k] * solved, axis=0, keepdims=True)
        ) * inverses[k]
        solved = jnp.where(positions == k, value, solved)
    out_ref[...] = jnp.zeros_like(out_ref)
    out_ref[:features, :] = -solved
    out_ref[features : features + 1, :] = forward_sq
    out_ref[features + 1 : features + 2, :] = grad_sq


def greet(partners):
    barrier = pltpu.get_barrier_semaphore()
    for partner in partners:
        pl.semaphore_signal(
            barrier, inc=1, device_id=partner, device_id_type=pl.DeviceIdType.MESH
        )
    pl.semaphore_wait(barrier, len(partners))


def share_steps(samples, ring, features, solved_ref, all_ref, sums_ref, got_ref, mine_ref, far_ref, sends, recvs):
    me, place = lax.axis_index("sample"), lax.axis_index("line")
    peers = [lax.rem(me + i, samples) for i in range(1, samples)]
    lines = [lax.rem(place + i, ring) for i in range(1, ring)]
    copies = []
    for slot, peer in enumerate(peers):
        copies.append(
            pltpu.make_async_remote_copy(
                src_ref=solved_ref,
                dst_ref=got_ref.at[slot],
                send_sem=sends.at[slot],
                recv_sem=recvs.at[slot],
                device_id={"sample": peer},
                device_id_type=pl.DeviceIdType.MESH,
            )
        )
        copies[-1].start()
    total = solved_ref[features:, :]
    for slot in range(samples - 1):
        copies[slot].wait_recv()
        total = total + got_ref[slot, features:, :]
    mine_ref[...] = total
    all_ref[me] = solved_ref[:features, :]
    for slot in range(samples - 1):
        source = lax.rem(me + samples - 1 - slot, samples)
        all_ref[source] = got_ref[slot, :features, :]
    far = []
    for slot, line in enumerate(lines):
        far.append(
            pltpu.make_async_remote_copy(
                src_ref=mine_ref,
                dst_ref=far_ref.at[slot],
                send_sem=sends.at[samples - 1 + slot],
                recv_sem=recvs.at[samples - 1 + slot],
                device_id={"line": line},
                device_id_type=pl.DeviceIdType.MESH,
            )
        )
        far[-1].start()
    total = mine_ref[...]
    for slot in range(ring - 1):
        far[slot].wait_recv()
        total = total + far_ref[slot]
    sums_ref[...] = total
    for copy in copies + far:
        copy.wait_send()


def split(value):
    top = value.astype(jnp.bfloat16)
    return top, (value - top.astype(jnp.float32)).astype(jnp.bfloat16)


def dot3(left, right):
    left_top, left_rest = split(left)
    right_top, right_rest = split(right)

    def product(a, b):
        return lax.dot_general(a, b, (((1,), (0,)), ((), ())), preferred_element_type=jnp.float32)

    return product(left_top, right_top) + (
        product(left_top, right_rest) + product(left_rest, right_top)
    )


def split_rows(width, total, ring):
    rows = (width + 15 + 15) // 16 * 16
    starts = [min(piece * width // 16 * 16, total - rows) for piece in range(ring)]
    return rows, starts


def newton_kernel(
    samples, ring, chunk, block, group,
    wind_ref, ptdf_ref, weights_ref, ends_ref, ratings_ref, monitored_ref, base_ref, cost_ref,
    policy_ref,
    policy_out, flow_out, size_out,
    diff_ref, factors_ref, all_ref, sums_ref, winds, grids, region_mix, stage, table, found, spread, outbox, inbox, mix_inbox,
    packed, weight_mine, policy_mine, cols, solved, step_inbox, mine, far,
    own_sem, stage_sems, send_up, recv_up, send_down, recv_down,
    send_out, recv_out, send_mix, recv_mix, send_step, recv_step,
):
    me, mine_s = lax.axis_index("line"), lax.axis_index("sample")
    regions = weights_ref.shape[0]
    features = regions + 1
    width, scen_here = wind_ref.shape
    total, lines_here = ptdf_ref.shape
    grid_lines = ends_ref.shape[1]
    share = lines_here // samples
    chunks = scen_here // chunk
    blocks = lines_here // block
    bands = (regions + 1) // 2
    reach = ring - 1
    f32, bf16 = jnp.float32, jnp.bfloat16
    peers = [lax.rem(mine_s + i, samples) for i in range(1, samples)]
    greet(
        [{"line": lax.rem(me + i, ring)} for i in range(1, ring)]
        + [{"sample": peer} for peer in peers]
    )

    def rows_of(step):
        return pl.ds(pl.multiple_of(step * chunk, chunk), chunk)

    def transfer(step, hops, side):
        piece = me - side * (hops - 1)
        slot = step * reach + hops - 1
        rows = rows_of(step)
        first = isinstance(hops, int) and hops == 1
        source = wind_ref.at[:, rows] if first else winds.at[piece, :, rows]
        sends_, recvs = (send_up, recv_up) if side == 1 else (send_down, recv_down)
        return pltpu.make_async_remote_copy(
            src_ref=source,
            dst_ref=winds.at[piece, :, rows],
            send_sem=sends_.at[slot],
            recv_sem=recvs.at[slot],
            device_id={"line": me + side},
            device_id_type=pl.DeviceIdType.MESH,
        )

    def transfer_first(step):
        for side in (1, -1):
            @pl.when(sends(1, side))
            def _():
                transfer(step, 1, side).wait_send()

    def sends(hops, side):
        if side == 1:
            return jnp.logical_and(me >= hops - 1, me < ring - 1)
        return jnp.logical_and(me <= ring - hops, me > 0)

    def receives(hops, side):
        return me >= hops if side == 1 else me < ring - hops

    def launch(step, hops):
        for side in (1, -1):
            @pl.when(sends(hops, side))
            def _():
                transfer(step, hops, side).start()

    def arrival(step, hops, side):
        slot = step * reach + hops - 1
        here = winds.at[me - side * hops, :, rows_of(step)]
        pltpu.make_async_remote_copy(
            src_ref=here,
            dst_ref=here,
            send_sem=(send_up if side == 1 else send_down).at[slot],
            recv_sem=(recv_up if side == 1 else recv_down).at[slot],
            device_id={"line": me - side},
            device_id_type=pl.DeviceIdType.MESH,
        ).wait_recv()

    launch(0, 1)
    if chunks > 1:
        launch(1, 1)
    own = pltpu.make_async_copy(wind_ref, winds.at[me], own_sem)
    own.start()

    stage_rows, starts = split_rows(width, total, ring)

    def staged(piece, index):
        slot = lax.rem(index, 2)
        return pltpu.make_async_copy(
            ptdf_ref.at[
                pl.ds(starts[piece], stage_rows), pl.ds(pl.multiple_of(index * block, block), block)
            ],
            stage.at[slot],
            stage_sems.at[slot],
        )

    region_mix[...] = jnp.zeros_like(region_mix)
    for piece in range(ring):
        region_mix[piece, :regions, :] = weights_ref[:, width * piece : width * (piece + 1)]
        skip = width * piece - starts[piece]
        staged(piece, 0).start()

        def place(index, carry):
            @pl.when(index + 1 < blocks)
            def _():
                staged(piece, index + 1).start()

            staged(piece, index).wait()
            lines = pl.ds(pl.multiple_of(index * block, block), block)
            grids[piece, :, lines] = stage[lax.rem(index, 2), skip : skip + width, :]
            return carry

        lax.fori_loop(0, blocks, place, 0)

    ends = ends_ref[...]
    rating_all = ratings_ref[...]
    first = rating_all.astype(bf16).astype(f32)
    second = (rating_all - first).astype(bf16).astype(f32)
    third = rating_all - first - second
    table[...] = jnp.zeros_like(table)
    table[:, :grid_lines] = jnp.concatenate(
        [
            (ends // 256).astype(f32),
            lax.rem(ends, 256).astype(f32),
            first,
            second,
            third,
            jnp.zeros_like(first),
        ],
        axis=0,
    ).astype(bf16)
    found[...] = jnp.zeros_like(found)

    def lookup(index, carry):
        where = pl.ds(pl.multiple_of(index * group, group), group)
        hot = (
            lax.broadcasted_iota(jnp.int32, (group, lines_here), 0) + index * group
            == monitored_ref[...]
        )
        found[...] += lax.dot_general(
            table[:, where],
            jnp.where(hot, 1.0, 0.0).astype(bf16),
            (((1,), (0,)), ((), ())),
            preferred_element_type=f32,
        )
        return carry

    lax.fori_loop(0, table.shape[1] // group, lookup, 0)
    from_bus = found[0:1, :] * 256.0 + found[2:3, :]
    to_bus = found[1:2, :] * 256.0 + found[3:4, :]
    rating_row = found[4:5, :] + found[5:6, :] + found[6:7, :]
    found[0:1, :] = from_bus
    found[1:2, :] = to_bus
    for d in range(samples):
        cut = slice(d * share, (d + 1) * share)
        spread[d, :features, :] = policy_ref[:, cut]
        spread[d, features : features + 1, :] = cost_ref[:, cut]
        spread[d, features + 1 : features + 2, :] = rating_row[:, cut]
    policy_mine[...] = spread[mine_s, :features, :]
    weight_mine[...] = spread[mine_s, features : features + 1, :] / (scen_here * samples)
    packed[...] = jnp.zeros_like(packed)
    own.wait()

    forward = (((1,), (0,)), ((), ()))

    def add_piece(step, piece):
        rows = rows_of(step)
        wind = winds[piece, :, rows]
        turned = wind.T
        buses = (
            lax.broadcasted_iota(jnp.int32, (width, block), 0) + piece * width
        ).astype(f32)

        def one(index, carry):
            lines = pl.ds(pl.multiple_of(index * block, block), block)
            pick = jnp.where(buses == found[1:2, lines], 1.0, 0.0) - jnp.where(
                buses == found[0:1, lines], 1.0, 0.0
            )
            grid = lax.dot_general(
                turned, grids[piece, :, lines], forward, preferred_element_type=f32
            )
            diff = lax.dot_general(
                turned, pick.astype(bf16), forward, preferred_element_type=f32
            )
            flow_out[rows, lines] += grid
            diff_ref[rows, lines] += diff
            return carry

        lax.fori_loop(0, blocks, one, 0)
        mix = lax.dot_general(region_mix[piece], wind, forward, preferred_element_type=f32)
        factors_ref[:, rows] += mix

    def finish(step):
        rows = rows_of(step)
        turned = factors_ref[:, rows].T
        mix_inbox[mine_s, step] = factors_ref[:, rows]
        diff = diff_ref[rows, :]
        flow = (
            flow_out[rows, :]
            + base_ref[...]
            + dot3(turned, policy_ref[...])
            + policy_ref[regions:, :] * diff
        )
        flow_out[rows, :] = flow
        for d in range(samples):
            cut = slice(d * share, (d + 1) * share)
            outbox[d, step, 0] = flow[:, cut].astype(bf16)
            outbox[d, step, 1] = diff[:, cut].astype(bf16)

    def parcel(step, slot, peer, source):
        spot = step * (samples - 1) + slot
        common = dict(device_id={"sample": peer}, device_id_type=pl.DeviceIdType.MESH)
        return (
            pltpu.make_async_remote_copy(
                src_ref=outbox.at[peer, step],
                dst_ref=inbox.at[source, step],
                send_sem=send_out.at[spot],
                recv_sem=recv_out.at[spot],
                **common,
            ),
            pltpu.make_async_remote_copy(
                src_ref=mix_inbox.at[mine_s, step],
                dst_ref=mix_inbox.at[source, step],
                send_sem=send_mix.at[spot],
                recv_sem=recv_mix.at[spot],
                **common,
            ),
        )

    def deliver(step):
        for slot, peer in enumerate(peers):
            for copy in parcel(step, slot, peer, mine_s):
                copy.start()

    def collect(step):
        inbox[mine_s, step] = outbox[mine_s, step]
        rating = spread[mine_s, features + 1 : features + 2, :]

        def one(turn, carry):
            source = lax.rem(mine_s + samples - turn, samples)

            @pl.when(turn > 0)
            def _():
                for copy in parcel(step, turn - 1, source, source):
                    copy.wait_recv()

            flow = inbox[source, step, 0].astype(f32)
            diff = inbox[source, step, 1].astype(f32)
            factors = mix_inbox[source, step]
            doubled = jnp.concatenate(
                [factors[:regions], factors[:regions], factors[regions:]], axis=0
            )
            pairs = jnp.concatenate(
                [doubled[d : d + features] * factors for d in range(bands)], axis=0
            )
            prob_up = jax.nn.sigmoid((flow - rating) / smoothing)
            prob_down = jax.nn.sigmoid((-flow - rating) / smoothing)
            slope = prob_up - prob_down
            curve = (prob_up * (1.0 - prob_up) + prob_down * (1.0 - prob_down)) / smoothing
            weighted = curve * diff
            top = bands * features
            packed[:top, :] += dot3(pairs, curve)
            packed[top : top + regions, :] += dot3(factors, weighted)[:regions]
            packed[top + regions : top + features, :] += jnp.sum(
                weighted * diff, axis=0, keepdims=True
            )
            low = top + features
            packed[low : low + regions, :] += dot3(factors, slope)[:regions]
            packed[low + regions : low + features, :] += jnp.sum(
                slope * diff, axis=0, keepdims=True
            )
            return carry

        lax.fori_loop(0, samples, one, 0)

    flow_out[...] = jnp.zeros_like(flow_out)
    diff_ref[...] = jnp.zeros_like(diff_ref)
    factors_ref[...] = jnp.zeros_like(factors_ref)

    def advance(step, carry):
        @pl.when(step + 2 < chunks)
        def _():
            launch(step + 2, 1)

        def visit(turn, inner):
            hops = (turn + 1) // 2

            @pl.when(lax.rem(turn, 2) == 1)
            def _():
                for side in (1, -1):
                    @pl.when(receives(hops, side))
                    def _():
                        arrival(step, hops, side)

                @pl.when(hops < reach)
                def _():
                    launch(step, hops + 1)

            piece = me + hops * (1 - 2 * lax.rem(turn, 2))

            @pl.when(jnp.logical_and(piece >= 0, piece < ring))
            def _():
                add_piece(step, piece)

            return inner

        lax.fori_loop(0, 2 * ring - 1, visit, 0)
        finish(step)
        deliver(step)

        @pl.when(step > 0)
        def _():
            collect(step - 1)

        return carry

    lax.fori_loop(0, chunks, advance, 0)
    collect(chunks - 1)
    solve_lines(regions, packed, weight_mine, policy_mine, solved, cols)
    share_steps(
        samples, ring, features, solved, all_ref, sums_ref, step_inbox, mine, far,
        send_step, recv_step,
    )
    sizes = jnp.sqrt(jnp.sum(sums_ref[...], axis=1, keepdims=True))
    size_out[...] = sizes[:2]
    scale = 1.0 / (
        1.0 + sizes[:1] / ((barrier_weight * features * lines_here * ring) ** 0.5)
    )
    scaled = scale * jnp.concatenate([all_ref[d] for d in range(samples)], axis=1)
    policy_out[...] = policy_ref[...] + scaled

    def update(step, carry):
        rows = rows_of(step)
        turned = factors_ref[:, rows].T
        flow_out[rows, :] += dot3(turned, scaled) + scaled[regions:, :] * diff_ref[rows, :]
        return carry

    lax.fori_loop(0, chunks, update, 0)

    def drain(step, carry):
        def line_drain(hops, inner):
            for side in (1, -1):
                @pl.when(sends(hops, side))
                def _():
                    transfer(step, hops, side).wait_send()
            return inner

        transfer_first(step)
        lax.fori_loop(2, ring, line_drain, 0)
        for slot, peer in enumerate(peers):
            for copy in parcel(step, slot, peer, mine_s):
                copy.wait_send()
        return carry

    lax.fori_loop(0, chunks, drain, 0)


def newton_steps(
    wind_dev, ptdf, region_weights, incidence, monitored, ratings, base_flow, line_cost, policy
):
    samples, ring = lax.axis_size("sample"), lax.axis_size("line")
    scen_here, width = wind_dev.shape
    lines_here, total = ptdf.shape
    features = policy.shape[0]
    share = lines_here // samples
    chunk = 128
    chunks = scen_here // chunk
    block = 256
    while lines_here % block:
        block //= 2
    group = 512
    table_cols = (incidence.shape[0] + group - 1) // group * group
    stage_rows, _ = split_rows(width, total, ring)
    packed_rows = (features // 2 + 2) * features
    hops = chunks * (ring - 1)
    parcels = chunks * (samples - 1)
    copies = samples + ring - 2
    vmem = pl.BlockSpec(memory_space=pltpu.VMEM)
    anywhere = pl.BlockSpec(memory_space=pl.ANY)
    f32, bf16 = jnp.float32, jnp.bfloat16
    dma = pltpu.SemaphoreType.DMA
    return pl.pallas_call(
        lambda *refs: newton_kernel(samples, ring, chunk, block, group, *refs),
        out_shape=(
            jax.ShapeDtypeStruct((features, lines_here), f32),
            jax.ShapeDtypeStruct((scen_here, lines_here), f32),
            jax.ShapeDtypeStruct((2, 1), f32),
        ),
        in_specs=[anywhere, anywhere] + [vmem] * 7,
        out_specs=(vmem,) * 3,
        scratch_shapes=[
            pltpu.VMEM((scen_here, lines_here), f32),
            pltpu.VMEM((features, scen_here), f32),
            pltpu.VMEM((samples, features, share), f32),
            pltpu.VMEM((8, share), f32),
            pltpu.VMEM((ring, width, scen_here), bf16),
            pltpu.VMEM((ring, width, lines_here), bf16),
            pltpu.VMEM((ring, features, width), bf16),
            pltpu.VMEM((2, stage_rows, block), bf16),
            pltpu.VMEM((8, table_cols), bf16),
            pltpu.VMEM((8, lines_here), f32),
            pltpu.VMEM((samples, features + 8, share), f32),
            pltpu.VMEM((samples, chunks, 2, chunk, share), bf16),
            pltpu.VMEM((samples, chunks, 2, chunk, share), bf16),
            pltpu.VMEM((samples, chunks, features, chunk), f32),
            pltpu.VMEM((packed_rows, share), f32),
            pltpu.VMEM((1, share), f32),
            pltpu.VMEM((features, share), f32),
            pltpu.VMEM((features, features, share), f32),
            pltpu.VMEM((features + 8, share), f32),
            pltpu.VMEM((samples - 1, features + 8, share), f32),
            pltpu.VMEM((8, share), f32),
            pltpu.VMEM((ring - 1, 8, share), f32),
            dma,
            dma((2,)),
            dma((hops,)),
            dma((hops,)),
            dma((hops,)),
            dma((hops,)),
            dma((parcels,)),
            dma((parcels,)),
            dma((parcels,)),
            dma((parcels,)),
            dma((copies,)),
            dma((copies,)),
        ],
        compiler_params=pltpu.CompilerParams(
            collective_id=0, has_side_effects=True, vmem_limit_bytes=67000000
        ),
        name="newton_steps",
    )(
        wind_dev.T, ptdf.T, region_weights, incidence.T, ratings[None, :], monitored[None, :],
        base_flow[None, :], line_cost[None, :], policy,
    )


def shards(*arrays):
    new_policy, new_flows, sizes = newton_steps(*arrays)
    return new_policy, new_flows, sizes[0, 0], sizes[1, 0]


def solution(mesh):
    placed = (
        P("sample", "line"),
        P("line", None),
        P(),
        P(),
        P("line"),
        P(),
        P("line"),
        P("line"),
        P(None, "line"),
    )
    return jax.shard_map(
        shards,
        mesh=mesh,
        in_specs=placed,
        out_specs=(P(None, "line"), P("sample", "line"), P(), P()),
        check_vma=False,
    )
```

```python
import jax
import jax.numpy as jnp
from jax import lax
from jax.experimental import pallas as pl
from jax.experimental.pallas import tpu as pltpu
from jax.sharding import PartitionSpec as P

ridge_weight = 1.0
barrier_weight = 0.1
smoothing = 0.5


def solve_lines(regions, packed_ref, weight_ref, policy_ref, out_ref, cols_ref):
    features = regions + 1
    weight = weight_ref[...]
    policy = policy_ref[...]
    margin_sq = 1.0 - policy * policy
    diag_terms = ridge_weight + barrier_weight * 2.0 * (1.0 + policy * policy) / (
        margin_sq * margin_sq
    )
    cols_ref[...] = jnp.zeros_like(cols_ref)
    bands = (regions + 1) // 2
    for band in range(bands):
        rows = packed_ref[band * features : (band + 1) * features, :] * weight
        if band == 0:
            rows = rows + diag_terms
        for i in range(regions):
            j = (i + band) % regions
            cols_ref[min(i, j), max(i, j) : max(i, j) + 1, :] = rows[i : i + 1]
    cross = packed_ref[bands * features : (bands + 1) * features, :] * weight
    for i in range(regions):
        cols_ref[i, regions : regions + 1, :] = cross[i : i + 1]
    cols_ref[regions, regions : regions + 1, :] = cross[regions:] + diag_terms[regions:]
    gradient = packed_ref[(bands + 1) * features : (bands + 2) * features, :] * weight
    gradient = gradient + ridge_weight * policy + barrier_weight * 2.0 * policy / margin_sq
    grad_sq = jnp.sum(gradient * gradient, axis=0, keepdims=True)

    positions = lax.broadcasted_iota(jnp.int32, gradient.shape, 0)
    inverses, forward = [], []
    running = gradient
    forward_sq = jnp.zeros_like(weight)
    for k in range(features):
        column = cols_ref[k]
        inverse = 1.0 / jnp.sqrt(column[k : k + 1])
        column = jnp.where(positions >= k, column * inverse, 0.0)
        cols_ref[k] = column
        value = running[k : k + 1] * inverse
        running = running - column * value
        forward_sq = forward_sq + value * value
        inverses.append(inverse)
        forward.append(value)
        for j in range(k + 1, features):
            base = j // 8 * 8
            cols_ref[j, base:, :] = cols_ref[j, base:, :] - column[base:] * column[j : j + 1]
    solved = jnp.zeros_like(gradient)
    for k in reversed(range(features)):
        value = (
            forward[k] - jnp.sum(cols_ref[k] * solved, axis=0, keepdims=True)
        ) * inverses[k]
        solved = jnp.where(positions == k, value, solved)
    out_ref[...] = jnp.zeros_like(out_ref)
    out_ref[:features, :] = -solved
    out_ref[features : features + 1, :] = forward_sq
    out_ref[features + 1 : features + 2, :] = grad_sq


def greet(partners):
    barrier = pltpu.get_barrier_semaphore()
    for partner in partners:
        pl.semaphore_signal(
            barrier, inc=1, device_id=partner, device_id_type=pl.DeviceIdType.MESH
        )
    pl.semaphore_wait(barrier, len(partners))


def share_steps(samples, ring, features, meanwhile, solved_ref, all_ref, sums_ref, got_ref, mine_ref, far_ref, sends, recvs):
    me, place = lax.axis_index("sample"), lax.axis_index("line")
    peers = [lax.rem(me + i, samples) for i in range(1, samples)]
    lines = [lax.rem(place + i, ring) for i in range(1, ring)]
    copies = []
    for slot, peer in enumerate(peers):
        copies.append(
            pltpu.make_async_remote_copy(
                src_ref=solved_ref,
                dst_ref=got_ref.at[slot],
                send_sem=sends.at[slot],
                recv_sem=recvs.at[slot],
                device_id={"sample": peer},
                device_id_type=pl.DeviceIdType.MESH,
            )
        )
        copies[-1].start()
    total = solved_ref[features:, :]
    for slot in range(samples - 1):
        copies[slot].wait_recv()
        total = total + got_ref[slot, features:, :]
    mine_ref[...] = total
    all_ref[me] = solved_ref[:features, :]
    for slot in range(samples - 1):
        source = lax.rem(me + samples - 1 - slot, samples)
        all_ref[source] = got_ref[slot, :features, :]
    far = []
    for slot, line in enumerate(lines):
        far.append(
            pltpu.make_async_remote_copy(
                src_ref=mine_ref,
                dst_ref=far_ref.at[slot],
                send_sem=sends.at[samples - 1 + slot],
                recv_sem=recvs.at[samples - 1 + slot],
                device_id={"line": line},
                device_id_type=pl.DeviceIdType.MESH,
            )
        )
        far[-1].start()
    meanwhile()
    total = mine_ref[...]
    for slot in range(ring - 1):
        far[slot].wait_recv()
        total = total + far_ref[slot]
    sums_ref[...] = total
    for copy in copies + far:
        copy.wait_send()


def split(value):
    top = value.astype(jnp.bfloat16)
    return top, (value - top.astype(jnp.float32)).astype(jnp.bfloat16)


def dot3(left, right):
    left_top, left_rest = split(left)
    right_top, right_rest = split(right)

    def product(a, b):
        return lax.dot_general(a, b, (((1,), (0,)), ((), ())), preferred_element_type=jnp.float32)

    return product(left_top, right_top) + (
        product(left_top, right_rest) + product(left_rest, right_top)
    )


def split_rows(width, total, ring):
    rows = (width + 15 + 15) // 16 * 16
    starts = [min(piece * width // 16 * 16, total - rows) for piece in range(ring)]
    return rows, starts


def newton_kernel(
    samples, ring, chunk, block, group,
    wind_ref, ptdf_ref, weights_hbm, ends_hbm, ratings_hbm, monitored_ref, base_ref, cost_ref,
    policy_ref,
    policy_out, flow_out, size_out,
    diff_ref, factors_ref, all_ref, sums_ref, winds, grids, region_mix, stage, table, found, spread, outbox, inbox, mix_inbox,
    packed, weight_mine, policy_mine, cols, solved, step_inbox, mine, far,
    own_sem, stage_sems, send_up, recv_up, send_down, recv_down,
    send_out, recv_out, send_mix, recv_mix, send_rest, recv_rest, send_step, recv_step,
    rest_out, rest_in, weights_ref, ends_ref, ratings_ref, small_sems,
):
    me, mine_s = lax.axis_index("line"), lax.axis_index("sample")
    regions = weights_hbm.shape[0]
    features = regions + 1
    width, scen_here = wind_ref.shape
    total, lines_here = ptdf_ref.shape
    grid_lines = ends_hbm.shape[1]
    share = lines_here // samples
    chunks = scen_here // chunk
    blocks = lines_here // block
    bands = (regions + 1) // 2
    reach = ring - 1
    f32, bf16 = jnp.float32, jnp.bfloat16
    peers = [lax.rem(mine_s + i, samples) for i in range(1, samples)]
    greet(
        [{"line": lax.rem(me + i, ring)} for i in range(1, ring)]
        + [{"sample": peer} for peer in peers]
    )

    def rows_of(step):
        return pl.ds(pl.multiple_of(step * chunk, chunk), chunk)

    middle = max(width // 2 // 16 * 16, 16)
    halves = ((0, middle), (middle, width - middle))
    ahead = 3

    def slot_of(step, hops, half):
        return (step * reach + hops - 1) * 2 + half

    def transfer(step, hops, side, half):
        piece = me - side * (hops - 1)
        slot = slot_of(step, hops, half)
        rows = rows_of(step)
        depth = pl.ds(*halves[half])
        first = isinstance(hops, int) and hops == 1
        source = wind_ref.at[depth, rows] if first else winds.at[piece, depth, rows]
        sends_, recvs = (send_up, recv_up) if side == 1 else (send_down, recv_down)
        return pltpu.make_async_remote_copy(
            src_ref=source,
            dst_ref=winds.at[piece, depth, rows],
            send_sem=sends_.at[slot],
            recv_sem=recvs.at[slot],
            device_id={"line": me + side},
            device_id_type=pl.DeviceIdType.MESH,
        )

    def sends(hops, side):
        if side == 1:
            return jnp.logical_and(me >= hops - 1, me < ring - 1)
        return jnp.logical_and(me <= ring - hops, me > 0)

    def receives(hops, side):
        return me >= hops if side == 1 else me < ring - hops

    def launch(step, hops, half):
        for side in (1, -1):
            @pl.when(sends(hops, side))
            def _():
                transfer(step, hops, side, half).start()

    def arrival(step, hops, side, half):
        slot = slot_of(step, hops, half)
        here = winds.at[me - side * hops, pl.ds(*halves[half]), rows_of(step)]
        pltpu.make_async_remote_copy(
            src_ref=here,
            dst_ref=here,
            send_sem=(send_up if side == 1 else send_down).at[slot],
            recv_sem=(recv_up if side == 1 else recv_down).at[slot],
            device_id={"line": me - side},
            device_id_type=pl.DeviceIdType.MESH,
        ).wait_recv()

    for step in range(min(chunks, ahead)):
        for half in (0, 1):
            launch(step, 1, half)
    own = pltpu.make_async_copy(wind_ref, winds.at[me], own_sem)
    own.start()

    small = [
        pltpu.make_async_copy(source, target, small_sems.at[index])
        for index, (source, target) in enumerate(
            [(weights_hbm, weights_ref), (ends_hbm, ends_ref), (ratings_hbm, ratings_ref)]
        )
    ]
    for copy in small:
        copy.start()
    stage_rows, starts = split_rows(width, total, ring)

    def staged(piece, index):
        slot = lax.rem(index, 2)
        return pltpu.make_async_copy(
            ptdf_ref.at[
                pl.ds(starts[piece], stage_rows), pl.ds(pl.multiple_of(index * block, block), block)
            ],
            stage.at[slot],
            stage_sems.at[slot],
        )

    region_mix[...] = jnp.zeros_like(region_mix)
    for copy in small:
        copy.wait()
    for piece in range(ring):
        region_mix[piece, :regions, :] = weights_ref[:, width * piece : width * (piece + 1)]
        skip = width * piece - starts[piece]
        staged(piece, 0).start()

        def place(index, carry):
            @pl.when(index + 1 < blocks)
            def _():
                staged(piece, index + 1).start()

            staged(piece, index).wait()
            lines = pl.ds(pl.multiple_of(index * block, block), block)
            grids[piece, :, lines] = stage[lax.rem(index, 2), skip : skip + width, :]
            return carry

        lax.fori_loop(0, blocks, place, 0)

    ends = ends_ref[...]
    rating_all = ratings_ref[...].reshape(1, grid_lines)
    first = rating_all.astype(bf16).astype(f32)
    second = (rating_all - first).astype(bf16).astype(f32)
    third = rating_all - first - second
    table[...] = jnp.zeros_like(table)
    table[:, :grid_lines] = jnp.concatenate(
        [
            (ends // 256).astype(f32),
            lax.rem(ends, 256).astype(f32),
            first,
            second,
            third,
            jnp.zeros_like(first),
        ],
        axis=0,
    ).astype(bf16)
    found[...] = jnp.zeros_like(found)

    def lookup(index, carry):
        where = pl.ds(pl.multiple_of(index * group, group), group)
        hot = (
            lax.broadcasted_iota(jnp.int32, (group, lines_here), 0) + index * group
            == monitored_ref[...]
        )
        found[...] += lax.dot_general(
            table[:, where],
            jnp.where(hot, 1.0, 0.0).astype(bf16),
            (((1,), (0,)), ((), ())),
            preferred_element_type=f32,
        )
        return carry

    lax.fori_loop(0, table.shape[1] // group, lookup, 0)
    from_bus = found[0:1, :] * 256.0 + found[2:3, :]
    to_bus = found[1:2, :] * 256.0 + found[3:4, :]
    rating_row = found[4:5, :] + found[5:6, :] + found[6:7, :]
    found[0:1, :] = from_bus
    found[1:2, :] = to_bus
    for d in range(samples):
        cut = slice(d * share, (d + 1) * share)
        spread[d, :features, :] = policy_ref[:, cut]
        spread[d, features : features + 1, :] = cost_ref[:, cut]
        spread[d, features + 1 : features + 2, :] = rating_row[:, cut]
    policy_mine[...] = spread[mine_s, :features, :]
    weight_mine[...] = spread[mine_s, features : features + 1, :] / (scen_here * samples)
    packed[...] = jnp.zeros_like(packed)
    own.wait()

    forward = (((1,), (0,)), ((), ()))

    def add_piece(step, piece, half):
        rows = rows_of(step)
        low, deep = halves[half]
        depth = pl.ds(low, deep)
        wind = winds[piece, depth, rows]
        turned = wind.T
        groups = [(cut, min(256, deep - cut)) for cut in range(0, deep, 256)]
        yes, no = bf16(1), bf16(0)

        def one(index, carry):
            lines = pl.ds(pl.multiple_of(index * block, block), block)
            local = found[0:2, lines] - (piece * width + low).astype(f32)
            picks = []
            for cut, size in groups:
                inside = local - float(cut)
                inside = jnp.where((inside >= 0) & (inside < size), inside, -1.0).astype(bf16)
                here = lax.broadcasted_iota(jnp.int32, (size, block), 0).astype(f32).astype(bf16)
                picks.append(
                    jnp.where(here == inside[1:2], yes, no)
                    - jnp.where(here == inside[0:1], yes, no)
                )
            flow_out[rows, lines] += lax.dot_general(
                turned, grids[piece, depth, lines], forward, preferred_element_type=f32
            )
            diff_ref[rows, lines] += lax.dot_general(
                turned, jnp.concatenate(picks, axis=0), forward, preferred_element_type=f32
            )
            return carry

        lax.fori_loop(0, blocks, one, 0)
        factors_ref[:, rows] += lax.dot_general(
            region_mix[piece, :, depth], wind, forward, preferred_element_type=f32
        )

    def finish(step):
        rows = rows_of(step)
        turned = factors_ref[:, rows].T
        mix_inbox[mine_s, step] = factors_ref[:, rows]
        diff = diff_ref[rows, :]
        flow = (
            flow_out[rows, :]
            + base_ref[...]
            + dot3(turned, policy_ref[...])
            + policy_ref[regions:, :] * diff
        )
        flow_out[rows, :] = flow
        for d in range(samples):
            cut = slice(d * share, (d + 1) * share)
            coarse = flow[:, cut].astype(bf16)
            outbox[d, step, 0] = coarse
            if chunks > 1:
                @pl.when(step < chunks - 1)
                def _():
                    rest_out[d, step] = (flow[:, cut] - coarse.astype(f32)).astype(bf16)

            outbox[d, step, 1] = diff[:, cut].astype(bf16)

    def parcel(step, slot, peer, source):
        spot = step * (samples - 1) + slot
        common = dict(device_id={"sample": peer}, device_id_type=pl.DeviceIdType.MESH)
        return (
            pltpu.make_async_remote_copy(
                src_ref=outbox.at[peer, step],
                dst_ref=inbox.at[source, step],
                send_sem=send_out.at[spot],
                recv_sem=recv_out.at[spot],
                **common,
            ),
            pltpu.make_async_remote_copy(
                src_ref=mix_inbox.at[mine_s, step],
                dst_ref=mix_inbox.at[source, step],
                send_sem=send_mix.at[spot],
                recv_sem=recv_mix.at[spot],
                **common,
            ),
        )

    def remainder(step, slot, peer, source):
        spot = step * (samples - 1) + slot
        return pltpu.make_async_remote_copy(
            src_ref=rest_out.at[peer, step],
            dst_ref=rest_in.at[source, step],
            send_sem=send_rest.at[spot],
            recv_sem=recv_rest.at[spot],
            device_id={"sample": peer},
            device_id_type=pl.DeviceIdType.MESH,
        )

    def deliver(step):
        for slot, peer in enumerate(peers):
            for copy in parcel(step, slot, peer, mine_s):
                copy.start()

        @pl.when(step < chunks - 1)
        def _():
            for slot, peer in enumerate(peers):
                remainder(step, slot, peer, mine_s).start()

    def collect(step, last):
        inbox[mine_s, step] = outbox[mine_s, step]
        if not last:
            rest_in[mine_s, step] = rest_out[mine_s, step]
        rating = spread[mine_s, features + 1 : features + 2, :]

        def one(turn, carry):
            source = lax.rem(mine_s + samples - turn, samples)

            @pl.when(turn > 0)
            def _():
                for copy in parcel(step, turn - 1, source, source):
                    copy.wait_recv()
                if not last:
                    remainder(step, turn - 1, source, source).wait_recv()

            flow = inbox[source, step, 0].astype(f32)
            if not last:
                flow = flow + rest_in[source, step].astype(f32)
            diff = inbox[source, step, 1].astype(f32)
            factors = mix_inbox[source, step]
            doubled = jnp.concatenate(
                [factors[:regions], factors[:regions], factors[regions:]], axis=0
            )
            pairs = jnp.concatenate(
                [doubled[d : d + features] * factors for d in range(bands)], axis=0
            )
            prob_up = jax.nn.sigmoid((flow - rating) / smoothing)
            prob_down = jax.nn.sigmoid((-flow - rating) / smoothing)
            slope = prob_up - prob_down
            curve = (prob_up * (1.0 - prob_up) + prob_down * (1.0 - prob_down)) / smoothing
            weighted = curve * diff
            top = bands * features
            packed[:top, :] += dot3(pairs, curve)
            packed[top : top + regions, :] += dot3(factors, weighted)[:regions]
            packed[top + regions : top + features, :] += jnp.sum(
                weighted * diff, axis=0, keepdims=True
            )
            low = top + features
            packed[low : low + regions, :] += dot3(factors, slope)[:regions]
            packed[low + regions : low + features, :] += jnp.sum(
                slope * diff, axis=0, keepdims=True
            )
            return carry

        lax.fori_loop(0, samples, one, 0)

    flow_out[...] = jnp.zeros_like(flow_out)
    diff_ref[...] = jnp.zeros_like(diff_ref)
    factors_ref[...] = jnp.zeros_like(factors_ref)

    def advance(tick, carry):
        @pl.when(tick + ahead < chunks)
        def _():
            for half in (0, 1):
                launch(tick + ahead, 1, half)

        def visit(turn, inner):
            hops = (turn + 1) // 2
            step = tick - jnp.maximum(hops - 1, 0)
            opening = lax.rem(turn, 2) == 1
            piece = me + hops * (1 - 2 * lax.rem(turn, 2))

            @pl.when(jnp.logical_and(step >= 0, step < chunks))
            def _():
                for half in (0, 1):
                    @pl.when(opening)
                    def _():
                        for side in (1, -1):
                            @pl.when(receives(hops, side))
                            def _():
                                arrival(step, hops, side, half)

                        @pl.when(hops < reach)
                        def _():
                            launch(step, hops + 1, half)

                    @pl.when(jnp.logical_and(piece >= 0, piece < ring))
                    def _():
                        add_piece(step, piece, half)

            return inner

        lax.fori_loop(0, 2 * ring - 1, visit, 0)
        done = tick - (reach - 1)

        @pl.when(done >= 0)
        def _():
            finish(done)
            deliver(done)

        @pl.when(done > 0)
        def _():
            collect(done - 1, False)

        return carry

    lax.fori_loop(0, chunks + reach - 1, advance, 0)
    collect(chunks - 1, True)
    solve_lines(regions, packed, weight_mine, policy_mine, solved, cols)
    def full_step():
        return jnp.concatenate([all_ref[d] for d in range(samples)], axis=1)

    def shifts():
        steps = full_step()

        def one(step, carry):
            rows = rows_of(step)
            turned = factors_ref[:, rows].T
            diff_ref[rows, :] = dot3(turned, steps) + steps[regions:, :] * diff_ref[rows, :]
            return carry

        lax.fori_loop(0, chunks, one, 0)

    share_steps(
        samples, ring, features, shifts, solved, all_ref, sums_ref, step_inbox, mine, far,
        send_step, recv_step,
    )
    sizes = jnp.sqrt(jnp.sum(sums_ref[...], axis=1, keepdims=True))
    size_out[...] = sizes[:2]
    scale = 1.0 / (
        1.0 + sizes[:1] / ((barrier_weight * features * lines_here * ring) ** 0.5)
    )
    policy_out[...] = policy_ref[...] + scale * full_step()
    flow_out[...] += scale * diff_ref[...]

    def drain(step, carry):
        def line_drain(hops, inner):
            for side in (1, -1):
                @pl.when(sends(hops, side))
                def _():
                    for half in (0, 1):
                        transfer(step, hops, side, half).wait_send()
            return inner

        for side in (1, -1):
            @pl.when(sends(1, side))
            def _():
                for half in (0, 1):
                    transfer(step, 1, side, half).wait_send()

        lax.fori_loop(2, ring, line_drain, 0)
        for slot, peer in enumerate(peers):
            for copy in parcel(step, slot, peer, mine_s):
                copy.wait_send()

        @pl.when(step < chunks - 1)
        def _():
            for slot, peer in enumerate(peers):
                remainder(step, slot, peer, mine_s).wait_send()

        return carry

    lax.fori_loop(0, chunks, drain, 0)


def newton_steps(
    wind_dev, ptdf, region_weights, incidence, monitored, ratings, base_flow, line_cost, policy
):
    samples, ring = lax.axis_size("sample"), lax.axis_size("line")
    scen_here, width = wind_dev.shape
    lines_here, total = ptdf.shape
    features = policy.shape[0]
    share = lines_here // samples
    chunk = 128
    chunks = scen_here // chunk
    block = 256
    while lines_here % block:
        block //= 2
    group = 512
    table_cols = (incidence.shape[0] + group - 1) // group * group
    stage_rows, _ = split_rows(width, total, ring)
    packed_rows = (features // 2 + 2) * features
    hops = 2 * chunks * (ring - 1)
    parcels = chunks * (samples - 1)
    copies = samples + ring - 2
    vmem = pl.BlockSpec(memory_space=pltpu.VMEM)
    anywhere = pl.BlockSpec(memory_space=pl.ANY)
    f32, bf16 = jnp.float32, jnp.bfloat16
    dma = pltpu.SemaphoreType.DMA
    return pl.pallas_call(
        lambda *refs: newton_kernel(samples, ring, chunk, block, group, *refs),
        out_shape=(
            jax.ShapeDtypeStruct((features, lines_here), f32),
            jax.ShapeDtypeStruct((scen_here, lines_here), f32),
            jax.ShapeDtypeStruct((2, 1), f32),
        ),
        in_specs=[anywhere] * 5 + [vmem] * 4,
        out_specs=(vmem,) * 3,
        scratch_shapes=[
            pltpu.VMEM((scen_here, lines_here), f32),
            pltpu.VMEM((features, scen_here), f32),
            pltpu.VMEM((samples, features, share), f32),
            pltpu.VMEM((8, share), f32),
            pltpu.VMEM((ring, width, scen_here), bf16),
            pltpu.VMEM((ring, width, lines_here), bf16),
            pltpu.VMEM((ring, features, width), bf16),
            pltpu.VMEM((2, stage_rows, block), bf16),
            pltpu.VMEM((8, table_cols), bf16),
            pltpu.VMEM((8, lines_here), f32),
            pltpu.VMEM((samples, features + 8, share), f32),
            pltpu.VMEM((samples, chunks, 2, chunk, share), bf16),
            pltpu.VMEM((samples, chunks, 2, chunk, share), bf16),
            pltpu.VMEM((samples, chunks, features, chunk), f32),
            pltpu.VMEM((packed_rows, share), f32),
            pltpu.VMEM((1, share), f32),
            pltpu.VMEM((features, share), f32),
            pltpu.VMEM((features, features, share), f32),
            pltpu.VMEM((features + 8, share), f32),
            pltpu.VMEM((samples - 1, features + 8, share), f32),
            pltpu.VMEM((8, share), f32),
            pltpu.VMEM((ring - 1, 8, share), f32),
            dma,
            dma((2,)),
            dma((hops,)),
            dma((hops,)),
            dma((hops,)),
            dma((hops,)),
            dma((parcels,)),
            dma((parcels,)),
            dma((parcels,)),
            dma((parcels,)),
            dma((parcels,)),
            dma((parcels,)),
            dma((copies,)),
            dma((copies,)),
            pltpu.VMEM((samples, chunks, chunk, share), bf16),
            pltpu.VMEM((samples, chunks, chunk, share), bf16),
            pltpu.VMEM(region_weights.shape, bf16),
            pltpu.VMEM(incidence.shape[::-1], jnp.int32),
            pltpu.VMEM(ratings.shape, f32),
            dma((3,)),
        ],
        compiler_params=pltpu.CompilerParams(
            collective_id=0, has_side_effects=True, vmem_limit_bytes=67000000
        ),
        name="newton_steps",
    )(
        wind_dev.T, ptdf.T, region_weights, incidence.T, ratings, monitored[None, :],
        base_flow[None, :], line_cost[None, :], policy,
    )


def hand_over(new_policy, new_flows, sizes):
    scen_here, lines_here = new_flows.shape
    rows = scen_here // 4

    def pass_on(policy_ref, flow_ref, sizes_ref, policy_out, flow_out, *size_outs):
        policy_out[...] = policy_ref[...]
        flow_out[...] = flow_ref[...]
        for row, size_out in enumerate(size_outs):
            size_out[...] = sizes_ref[row : row + 1, :]

    def whole(shape):
        return pl.BlockSpec(shape, lambda step: (0, 0))

    flow_block = pl.BlockSpec((rows, lines_here), lambda step: (step, 0))
    return pl.pallas_call(
        pass_on,
        grid=(4,),
        in_specs=[whole(new_policy.shape), flow_block, whole(sizes.shape)],
        out_specs=(whole(new_policy.shape), flow_block, whole((1, 1)), whole((1, 1))),
        out_shape=(
            jax.ShapeDtypeStruct(new_policy.shape, jnp.float32),
            jax.ShapeDtypeStruct(new_flows.shape, jnp.float32),
            jax.ShapeDtypeStruct((1, 1), jnp.float32),
            jax.ShapeDtypeStruct((1, 1), jnp.float32),
        ),
        name="hand_over",
    )(new_policy, new_flows, sizes)


def shards(*arrays):
    new_policy, new_flows, decrement, grad_norm = hand_over(*newton_steps(*arrays))
    return new_policy, new_flows, decrement.reshape(()), grad_norm.reshape(())


def solution(mesh):
    placed = (
        P("sample", "line"),
        P("line", None),
        P(),
        P(),
        P("line"),
        P(),
        P("line"),
        P("line"),
        P(None, "line"),
    )
    return jax.shard_map(
        shards,
        mesh=mesh,
        in_specs=placed,
        out_specs=(P(None, "line"), P("sample", "line"), P(), P()),
        check_vma=False,
    )
```

```python
import jax
import jax.numpy as jnp
from jax import lax
from jax.experimental import pallas as pl
from jax.experimental.pallas import tpu as pltpu
from jax.sharding import PartitionSpec as P

ridge_weight = 1.0
barrier_weight = 0.1
smoothing = 0.5


def solve_lines(regions, packed_ref, weight_ref, policy_ref, out_ref, cols_ref):
    features = regions + 1
    weight = weight_ref[...]
    policy = policy_ref[...]
    margin_sq = 1.0 - policy * policy
    diag_terms = ridge_weight + barrier_weight * 2.0 * (1.0 + policy * policy) / (
        margin_sq * margin_sq
    )
    cols_ref[...] = jnp.zeros_like(cols_ref)
    bands = (regions + 1) // 2
    for band in range(bands):
        rows = packed_ref[band * features : (band + 1) * features, :] * weight
        if band == 0:
            rows = rows + diag_terms
        for i in range(regions):
            j = (i + band) % regions
            cols_ref[min(i, j), max(i, j) : max(i, j) + 1, :] = rows[i : i + 1]
    cross = packed_ref[bands * features : (bands + 1) * features, :] * weight
    for i in range(regions):
        cols_ref[i, regions : regions + 1, :] = cross[i : i + 1]
    cols_ref[regions, regions : regions + 1, :] = cross[regions:] + diag_terms[regions:]
    gradient = packed_ref[(bands + 1) * features : (bands + 2) * features, :] * weight
    gradient = gradient + ridge_weight * policy + barrier_weight * 2.0 * policy / margin_sq
    grad_sq = jnp.sum(gradient * gradient, axis=0, keepdims=True)

    positions = lax.broadcasted_iota(jnp.int32, gradient.shape, 0)
    inverses, forward = [], []
    running = gradient
    forward_sq = jnp.zeros_like(weight)
    for k in range(features):
        column = cols_ref[k]
        inverse = 1.0 / jnp.sqrt(column[k : k + 1])
        column = jnp.where(positions >= k, column * inverse, 0.0)
        cols_ref[k] = column
        value = running[k : k + 1] * inverse
        running = running - column * value
        forward_sq = forward_sq + value * value
        inverses.append(inverse)
        forward.append(value)
        for j in range(k + 1, features):
            base = j // 8 * 8
            cols_ref[j, base:, :] = cols_ref[j, base:, :] - column[base:] * column[j : j + 1]
    solved = jnp.zeros_like(gradient)
    for k in reversed(range(features)):
        value = (
            forward[k] - jnp.sum(cols_ref[k] * solved, axis=0, keepdims=True)
        ) * inverses[k]
        solved = jnp.where(positions == k, value, solved)
    out_ref[...] = jnp.zeros_like(out_ref)
    out_ref[:features, :] = -solved
    out_ref[features : features + 1, :] = forward_sq
    out_ref[features + 1 : features + 2, :] = grad_sq


def greet(partners):
    barrier = pltpu.get_barrier_semaphore()
    for partner in partners:
        pl.semaphore_signal(
            barrier, inc=1, device_id=partner, device_id_type=pl.DeviceIdType.MESH
        )
    pl.semaphore_wait(barrier, len(partners))


def share_steps(samples, ring, features, meanwhile, solved_ref, all_ref, sums_ref, got_ref, mine_ref, far_ref, sends, recvs):
    me, place = lax.axis_index("sample"), lax.axis_index("line")
    peers = [lax.rem(me + i, samples) for i in range(1, samples)]
    lines = [lax.rem(place + i, ring) for i in range(1, ring)]
    copies = []
    for slot, peer in enumerate(peers):
        copies.append(
            pltpu.make_async_remote_copy(
                src_ref=solved_ref,
                dst_ref=got_ref.at[slot],
                send_sem=sends.at[slot],
                recv_sem=recvs.at[slot],
                device_id={"sample": peer},
                device_id_type=pl.DeviceIdType.MESH,
            )
        )
        copies[-1].start()
    total = solved_ref[features:, :]
    for slot in range(samples - 1):
        copies[slot].wait_recv()
        total = total + got_ref[slot, features:, :]
    mine_ref[...] = total
    all_ref[me] = solved_ref[:features, :]
    for slot in range(samples - 1):
        source = lax.rem(me + samples - 1 - slot, samples)
        all_ref[source] = got_ref[slot, :features, :]
    far = []
    for slot, line in enumerate(lines):
        far.append(
            pltpu.make_async_remote_copy(
                src_ref=mine_ref,
                dst_ref=far_ref.at[slot],
                send_sem=sends.at[samples - 1 + slot],
                recv_sem=recvs.at[samples - 1 + slot],
                device_id={"line": line},
                device_id_type=pl.DeviceIdType.MESH,
            )
        )
        far[-1].start()
    meanwhile()
    total = mine_ref[...]
    for slot in range(ring - 1):
        far[slot].wait_recv()
        total = total + far_ref[slot]
    sums_ref[...] = total
    for copy in copies + far:
        copy.wait_send()


def split(value):
    top = value.astype(jnp.bfloat16)
    return top, (value - top.astype(jnp.float32)).astype(jnp.bfloat16)


def dot3(left, right):
    left_top, left_rest = split(left)
    right_top, right_rest = split(right)

    def product(a, b):
        return lax.dot_general(a, b, (((1,), (0,)), ((), ())), preferred_element_type=jnp.float32)

    return product(left_top, right_top) + (
        product(left_top, right_rest) + product(left_rest, right_top)
    )


def split_rows(width, total, ring):
    rows = (width + 15 + 15) // 16 * 16
    starts = [min(piece * width // 16 * 16, total - rows) for piece in range(ring)]
    return rows, starts


def newton_kernel(
    samples, ring, chunk, block, group,
    wind_ref, ptdf_ref, weights_hbm, ends_hbm, ratings_hbm, monitored_hbm, base_hbm, cost_hbm,
    policy_hbm,
    policy_out, flow_out, decrement_out, norm_out,
    diff_ref, factors_ref, all_ref, sums_ref, winds, grids, region_mix, stage, table, found, spread, outbox, inbox, mix_inbox,
    packed, weight_mine, policy_mine, cols, solved, step_inbox, mine, far,
    own_sem, stage_sems, send_up, recv_up, send_down, recv_down,
    send_out, recv_out, send_mix, recv_mix, send_rest, recv_rest, send_step, recv_step,
    rest_out, rest_in, weights_ref, ends_ref, ratings_ref, monitored_ref, base_ref, cost_ref,
    policy_ref, small_sems,
):
    me, mine_s = lax.axis_index("line"), lax.axis_index("sample")
    regions = weights_hbm.shape[0]
    features = regions + 1
    width, scen_here = wind_ref.shape
    total, lines_here = ptdf_ref.shape
    grid_lines = ends_hbm.shape[1]
    share = lines_here // samples
    chunks = scen_here // chunk
    blocks = lines_here // block
    bands = (regions + 1) // 2
    reach = ring - 1
    f32, bf16 = jnp.float32, jnp.bfloat16
    peers = [lax.rem(mine_s + i, samples) for i in range(1, samples)]
    greet(
        [{"line": lax.rem(me + i, ring)} for i in range(1, ring)]
        + [{"sample": peer} for peer in peers]
    )

    def rows_of(step):
        return pl.ds(pl.multiple_of(step * chunk, chunk), chunk)

    middle = max(width // 2 // 16 * 16, 16)
    halves = ((0, middle), (middle, width - middle))
    ahead = 3

    def slot_of(step, hops, half):
        return (step * reach + hops - 1) * 2 + half

    def transfer(step, hops, side, half):
        piece = me - side * (hops - 1)
        slot = slot_of(step, hops, half)
        rows = rows_of(step)
        depth = pl.ds(*halves[half])
        first = isinstance(hops, int) and hops == 1
        source = wind_ref.at[depth, rows] if first else winds.at[piece, depth, rows]
        sends_, recvs = (send_up, recv_up) if side == 1 else (send_down, recv_down)
        return pltpu.make_async_remote_copy(
            src_ref=source,
            dst_ref=winds.at[piece, depth, rows],
            send_sem=sends_.at[slot],
            recv_sem=recvs.at[slot],
            device_id={"line": me + side},
            device_id_type=pl.DeviceIdType.MESH,
        )

    def sends(hops, side):
        if side == 1:
            return jnp.logical_and(me >= hops - 1, me < ring - 1)
        return jnp.logical_and(me <= ring - hops, me > 0)

    def receives(hops, side):
        return me >= hops if side == 1 else me < ring - hops

    def launch(step, hops, half):
        for side in (1, -1):
            @pl.when(sends(hops, side))
            def _():
                transfer(step, hops, side, half).start()

    def arrival(step, hops, side, half):
        slot = slot_of(step, hops, half)
        here = winds.at[me - side * hops, pl.ds(*halves[half]), rows_of(step)]
        pltpu.make_async_remote_copy(
            src_ref=here,
            dst_ref=here,
            send_sem=(send_up if side == 1 else send_down).at[slot],
            recv_sem=(recv_up if side == 1 else recv_down).at[slot],
            device_id={"line": me - side},
            device_id_type=pl.DeviceIdType.MESH,
        ).wait_recv()

    for step in range(min(chunks, ahead)):
        for half in (0, 1):
            launch(step, 1, half)
    own = pltpu.make_async_copy(wind_ref, winds.at[me], own_sem)
    own.start()

    small = [
        pltpu.make_async_copy(source, target, small_sems.at[index])
        for index, (source, target) in enumerate(
            [
                (weights_hbm, weights_ref),
                (ends_hbm, ends_ref),
                (ratings_hbm, ratings_ref),
                (monitored_hbm, monitored_ref),
                (base_hbm, base_ref),
                (cost_hbm, cost_ref),
                (policy_hbm, policy_ref),
            ]
        )
    ]
    for copy in small:
        copy.start()
    stage_rows, starts = split_rows(width, total, ring)

    def staged(piece, index):
        slot = lax.rem(index, 2)
        return pltpu.make_async_copy(
            ptdf_ref.at[
                pl.ds(starts[piece], stage_rows), pl.ds(pl.multiple_of(index * block, block), block)
            ],
            stage.at[slot],
            stage_sems.at[slot],
        )

    region_mix[...] = jnp.zeros_like(region_mix)
    for copy in small:
        copy.wait()
    for piece in range(ring):
        region_mix[piece, :regions, :] = weights_ref[:, width * piece : width * (piece + 1)]
        skip = width * piece - starts[piece]
        staged(piece, 0).start()

        def place(index, carry):
            @pl.when(index + 1 < blocks)
            def _():
                staged(piece, index + 1).start()

            staged(piece, index).wait()
            lines = pl.ds(pl.multiple_of(index * block, block), block)
            grids[piece, :, lines] = stage[lax.rem(index, 2), skip : skip + width, :]
            return carry

        lax.fori_loop(0, blocks, place, 0)

    ends = ends_ref[...]
    rating_all = ratings_ref[...].reshape(1, grid_lines)
    first = rating_all.astype(bf16).astype(f32)
    second = (rating_all - first).astype(bf16).astype(f32)
    third = rating_all - first - second
    table[...] = jnp.zeros_like(table)
    table[:, :grid_lines] = jnp.concatenate(
        [
            (ends // 256).astype(f32),
            lax.rem(ends, 256).astype(f32),
            first,
            second,
            third,
            jnp.zeros_like(first),
        ],
        axis=0,
    ).astype(bf16)
    found[...] = jnp.zeros_like(found)

    def lookup(index, carry):
        where = pl.ds(pl.multiple_of(index * group, group), group)
        hot = (
            lax.broadcasted_iota(jnp.int32, (group, lines_here), 0) + index * group
            == monitored_ref[...]
        )
        found[...] += lax.dot_general(
            table[:, where],
            jnp.where(hot, 1.0, 0.0).astype(bf16),
            (((1,), (0,)), ((), ())),
            preferred_element_type=f32,
        )
        return carry

    lax.fori_loop(0, table.shape[1] // group, lookup, 0)
    from_bus = found[0:1, :] * 256.0 + found[2:3, :]
    to_bus = found[1:2, :] * 256.0 + found[3:4, :]
    rating_row = found[4:5, :] + found[5:6, :] + found[6:7, :]
    found[0:1, :] = from_bus
    found[1:2, :] = to_bus
    for d in range(samples):
        cut = slice(d * share, (d + 1) * share)
        spread[d, :features, :] = policy_ref[:, cut]
        spread[d, features : features + 1, :] = cost_ref[:, cut]
        spread[d, features + 1 : features + 2, :] = rating_row[:, cut]
    policy_mine[...] = spread[mine_s, :features, :]
    weight_mine[...] = spread[mine_s, features : features + 1, :] / (scen_here * samples)
    packed[...] = jnp.zeros_like(packed)
    own.wait()

    forward = (((1,), (0,)), ((), ()))

    def add_piece(step, piece, half):
        rows = rows_of(step)
        low, deep = halves[half]
        depth = pl.ds(low, deep)
        wind = winds[piece, depth, rows]
        turned = wind.T
        groups = [(cut, min(256, deep - cut)) for cut in range(0, deep, 256)]
        yes, no = bf16(1), bf16(0)

        def one(index, carry):
            lines = pl.ds(pl.multiple_of(index * block, block), block)
            local = found[0:2, lines] - (piece * width + low).astype(f32)
            picks = []
            for cut, size in groups:
                inside = local - float(cut)
                inside = jnp.where((inside >= 0) & (inside < size), inside, -1.0).astype(bf16)
                here = lax.broadcasted_iota(jnp.int32, (size, block), 0).astype(f32).astype(bf16)
                picks.append(
                    jnp.where(here == inside[1:2], yes, no)
                    - jnp.where(here == inside[0:1], yes, no)
                )
            flow_out[rows, lines] += lax.dot_general(
                turned, grids[piece, depth, lines], forward, preferred_element_type=f32
            )
            diff_ref[rows, lines] += lax.dot_general(
                turned, jnp.concatenate(picks, axis=0), forward, preferred_element_type=f32
            )
            return carry

        lax.fori_loop(0, blocks, one, 0)
        factors_ref[:, rows] += lax.dot_general(
            region_mix[piece, :, depth], wind, forward, preferred_element_type=f32
        )

    def finish(step):
        rows = rows_of(step)
        turned = factors_ref[:, rows].T
        mix_inbox[mine_s, step] = factors_ref[:, rows]
        diff = diff_ref[rows, :]
        flow = (
            flow_out[rows, :]
            + base_ref[...]
            + dot3(turned, policy_ref[...])
            + policy_ref[regions:, :] * diff
        )
        flow_out[rows, :] = flow
        for d in range(samples):
            cut = slice(d * share, (d + 1) * share)
            coarse = flow[:, cut].astype(bf16)
            outbox[d, step, 0] = coarse
            if chunks > 1:
                @pl.when(step < chunks - 1)
                def _():
                    rest_out[d, step] = (flow[:, cut] - coarse.astype(f32)).astype(bf16)

            outbox[d, step, 1] = diff[:, cut].astype(bf16)

    def parcel(step, slot, peer, source):
        spot = step * (samples - 1) + slot
        common = dict(device_id={"sample": peer}, device_id_type=pl.DeviceIdType.MESH)
        return (
            pltpu.make_async_remote_copy(
                src_ref=outbox.at[peer, step],
                dst_ref=inbox.at[source, step],
                send_sem=send_out.at[spot],
                recv_sem=recv_out.at[spot],
                **common,
            ),
            pltpu.make_async_remote_copy(
                src_ref=mix_inbox.at[mine_s, step],
                dst_ref=mix_inbox.at[source, step],
                send_sem=send_mix.at[spot],
                recv_sem=recv_mix.at[spot],
                **common,
            ),
        )

    def remainder(step, slot, peer, source):
        spot = step * (samples - 1) + slot
        return pltpu.make_async_remote_copy(
            src_ref=rest_out.at[peer, step],
            dst_ref=rest_in.at[source, step],
            send_sem=send_rest.at[spot],
            recv_sem=recv_rest.at[spot],
            device_id={"sample": peer},
            device_id_type=pl.DeviceIdType.MESH,
        )

    def deliver(step):
        for slot, peer in enumerate(peers):
            for copy in parcel(step, slot, peer, mine_s):
                copy.start()

        @pl.when(step < chunks - 1)
        def _():
            for slot, peer in enumerate(peers):
                remainder(step, slot, peer, mine_s).start()

    def collect(step, last):
        inbox[mine_s, step] = outbox[mine_s, step]
        if not last:
            rest_in[mine_s, step] = rest_out[mine_s, step]
        rating = spread[mine_s, features + 1 : features + 2, :]

        batch = 2 if samples % 2 == 0 else 1

        def one(turn, carry):
            flows, diffs, mixes = [], [], []
            for inner in range(batch):
                order = turn * batch + inner
                source = lax.rem(mine_s + samples - order, samples)

                @pl.when(order > 0)
                def _():
                    for copy in parcel(step, order - 1, source, source):
                        copy.wait_recv()
                    if not last:
                        remainder(step, order - 1, source, source).wait_recv()

                flow = inbox[source, step, 0].astype(f32)
                if not last:
                    flow = flow + rest_in[source, step].astype(f32)
                flows.append(flow)
                diffs.append(inbox[source, step, 1].astype(f32))
                mixes.append(mix_inbox[source, step])
            flow = jnp.concatenate(flows, axis=0)
            diff = jnp.concatenate(diffs, axis=0)
            factors = jnp.concatenate(mixes, axis=1)
            doubled = jnp.concatenate(
                [factors[:regions], factors[:regions], factors[regions:]], axis=0
            )
            pairs = jnp.concatenate(
                [doubled[d : d + features] * factors for d in range(bands)], axis=0
            )
            prob_up = jax.nn.sigmoid((flow - rating) / smoothing)
            prob_down = jax.nn.sigmoid((-flow - rating) / smoothing)
            slope = prob_up - prob_down
            curve = (prob_up * (1.0 - prob_up) + prob_down * (1.0 - prob_down)) / smoothing
            weighted = curve * diff
            top = bands * features
            low = top + features
            packed[:top, :] += dot3(pairs, curve)
            packed[top : top + regions, :] += dot3(factors, weighted)[:regions]
            packed[top + regions : low, :] += jnp.sum(weighted * diff, axis=0, keepdims=True)
            packed[low : low + regions, :] += dot3(factors, slope)[:regions]
            packed[low + regions : low + features, :] += jnp.sum(
                slope * diff, axis=0, keepdims=True
            )
            return carry

        lax.fori_loop(0, samples // batch, one, 0)

    flow_out[...] = jnp.zeros_like(flow_out)
    diff_ref[...] = jnp.zeros_like(diff_ref)
    factors_ref[...] = jnp.zeros_like(factors_ref)

    def advance(tick, carry):
        @pl.when(tick + ahead < chunks)
        def _():
            for half in (0, 1):
                launch(tick + ahead, 1, half)

        def visit(turn, inner):
            hops = (turn + 1) // 2
            step = tick - jnp.maximum(hops - 1, 0)
            opening = lax.rem(turn, 2) == 1
            piece = me + hops * (1 - 2 * lax.rem(turn, 2))

            @pl.when(jnp.logical_and(step >= 0, step < chunks))
            def _():
                for half in (0, 1):
                    @pl.when(opening)
                    def _():
                        for side in (1, -1):
                            @pl.when(receives(hops, side))
                            def _():
                                arrival(step, hops, side, half)

                        @pl.when(hops < reach)
                        def _():
                            launch(step, hops + 1, half)

                    @pl.when(jnp.logical_and(piece >= 0, piece < ring))
                    def _():
                        add_piece(step, piece, half)

            return inner

        lax.fori_loop(0, 2 * ring - 1, visit, 0)
        done = tick - (reach - 1)

        @pl.when(done >= 0)
        def _():
            finish(done)
            deliver(done)

        @pl.when(done > 0)
        def _():
            collect(done - 1, False)

        return carry

    lax.fori_loop(0, chunks + reach - 1, advance, 0)
    collect(chunks - 1, True)
    solve_lines(regions, packed, weight_mine, policy_mine, solved, cols)
    def full_step():
        return jnp.concatenate([all_ref[d] for d in range(samples)], axis=1)

    def shifts():
        steps = full_step()

        def one(step, carry):
            rows = rows_of(step)
            turned = factors_ref[:, rows].T
            diff_ref[rows, :] = dot3(turned, steps) + steps[regions:, :] * diff_ref[rows, :]
            return carry

        lax.fori_loop(0, chunks, one, 0)

    share_steps(
        samples, ring, features, shifts, solved, all_ref, sums_ref, step_inbox, mine, far,
        send_step, recv_step,
    )
    sizes = jnp.sqrt(jnp.sum(sums_ref[...], axis=1, keepdims=True))
    decrement_out[...] = sizes[:1]
    norm_out[...] = sizes[1:2]
    scale = 1.0 / (
        1.0 + sizes[:1] / ((barrier_weight * features * lines_here * ring) ** 0.5)
    )
    policy_out[...] = policy_ref[...] + scale * full_step()
    flow_out[...] += scale * diff_ref[...]

    def drain(step, carry):
        def line_drain(hops, inner):
            for side in (1, -1):
                @pl.when(sends(hops, side))
                def _():
                    for half in (0, 1):
                        transfer(step, hops, side, half).wait_send()
            return inner

        for side in (1, -1):
            @pl.when(sends(1, side))
            def _():
                for half in (0, 1):
                    transfer(step, 1, side, half).wait_send()

        lax.fori_loop(2, ring, line_drain, 0)
        for slot, peer in enumerate(peers):
            for copy in parcel(step, slot, peer, mine_s):
                copy.wait_send()

        @pl.when(step < chunks - 1)
        def _():
            for slot, peer in enumerate(peers):
                remainder(step, slot, peer, mine_s).wait_send()

        return carry

    lax.fori_loop(0, chunks, drain, 0)


def newton_steps(
    wind_dev, ptdf, region_weights, incidence, monitored, ratings, base_flow, line_cost, policy
):
    samples, ring = lax.axis_size("sample"), lax.axis_size("line")
    scen_here, width = wind_dev.shape
    lines_here, total = ptdf.shape
    features = policy.shape[0]
    share = lines_here // samples
    chunk = 128
    chunks = scen_here // chunk
    block = 256
    while lines_here % block:
        block //= 2
    group = 512
    table_cols = (incidence.shape[0] + group - 1) // group * group
    stage_rows, _ = split_rows(width, total, ring)
    packed_rows = (features // 2 + 2) * features
    hops = 2 * chunks * (ring - 1)
    parcels = chunks * (samples - 1)
    copies = samples + ring - 2
    vmem = pl.BlockSpec(memory_space=pltpu.VMEM)
    far_off = pl.BlockSpec(memory_space=pltpu.HBM)
    f32, bf16 = jnp.float32, jnp.bfloat16
    dma = pltpu.SemaphoreType.DMA
    return pl.pallas_call(
        lambda *refs: newton_kernel(samples, ring, chunk, block, group, *refs),
        out_shape=(
            pltpu.VMEM((features, lines_here), f32),
            pltpu.VMEM((scen_here, lines_here), f32),
            pltpu.VMEM((1, 1), f32),
            pltpu.VMEM((1, 1), f32),
        ),
        in_specs=[far_off] * 9,
        out_specs=(vmem,) * 4,
        scratch_shapes=[
            pltpu.VMEM((scen_here, lines_here), f32),
            pltpu.VMEM((features, scen_here), f32),
            pltpu.VMEM((samples, features, share), f32),
            pltpu.VMEM((8, share), f32),
            pltpu.VMEM((ring, width, scen_here), bf16),
            pltpu.VMEM((ring, width, lines_here), bf16),
            pltpu.VMEM((ring, features, width), bf16),
            pltpu.VMEM((2, stage_rows, block), bf16),
            pltpu.VMEM((8, table_cols), bf16),
            pltpu.VMEM((8, lines_here), f32),
            pltpu.VMEM((samples, features + 8, share), f32),
            pltpu.VMEM((samples, chunks, 2, chunk, share), bf16),
            pltpu.VMEM((samples, chunks, 2, chunk, share), bf16),
            pltpu.VMEM((samples, chunks, features, chunk), f32),
            pltpu.VMEM((packed_rows, share), f32),
            pltpu.VMEM((1, share), f32),
            pltpu.VMEM((features, share), f32),
            pltpu.VMEM((features, features, share), f32),
            pltpu.VMEM((features + 8, share), f32),
            pltpu.VMEM((samples - 1, features + 8, share), f32),
            pltpu.VMEM((8, share), f32),
            pltpu.VMEM((ring - 1, 8, share), f32),
            dma,
            dma((2,)),
            dma((hops,)),
            dma((hops,)),
            dma((hops,)),
            dma((hops,)),
            dma((parcels,)),
            dma((parcels,)),
            dma((parcels,)),
            dma((parcels,)),
            dma((parcels,)),
            dma((parcels,)),
            dma((copies,)),
            dma((copies,)),
            pltpu.VMEM((samples, chunks, chunk, share), bf16),
            pltpu.VMEM((samples, chunks, chunk, share), bf16),
            pltpu.VMEM(region_weights.shape, bf16),
            pltpu.VMEM(incidence.shape[::-1], jnp.int32),
            pltpu.VMEM(ratings.shape, f32),
            pltpu.VMEM((1, lines_here), jnp.int32),
            pltpu.VMEM((1, lines_here), f32),
            pltpu.VMEM((1, lines_here), f32),
            pltpu.VMEM(policy.shape, f32),
            dma((7,)),
        ],
        compiler_params=pltpu.CompilerParams(
            collective_id=0, has_side_effects=True, vmem_limit_bytes=60000000
        ),
        name="newton_steps",
    )(
        wind_dev.T, ptdf.T, region_weights, incidence.T, ratings, monitored[None, :],
        base_flow[None, :], line_cost[None, :], policy,
    )


def shards(*arrays):
    new_policy, new_flows, decrement, grad_norm = newton_steps(*arrays)
    return new_policy, new_flows, decrement.reshape(()), grad_norm.reshape(())


def solution(mesh):
    placed = (
        P("sample", "line"),
        P("line", None),
        P(),
        P(),
        P("line"),
        P(),
        P("line"),
        P("line"),
        P(None, "line"),
    )
    return jax.shard_map(
        shards,
        mesh=mesh,
        in_specs=placed,
        out_specs=(P(None, "line"), P("sample", "line"), P(), P()),
        check_vma=False,
    )
```

```python
import jax
import jax.numpy as jnp
from jax import lax
from jax.experimental import pallas as pl
from jax.experimental.pallas import tpu as pltpu
from jax.sharding import PartitionSpec as P

ridge_weight = 1.0
barrier_weight = 0.1
smoothing = 0.5


def solve_lines(regions, packed_ref, weight_ref, policy_ref, out_ref, cols_ref):
    features = regions + 1
    weight = weight_ref[...]
    policy = policy_ref[...]
    margin_sq = 1.0 - policy * policy
    diag_terms = ridge_weight + barrier_weight * 2.0 * (1.0 + policy * policy) / (
        margin_sq * margin_sq
    )
    cols_ref[...] = jnp.zeros_like(cols_ref)
    bands = (regions + 1) // 2
    for band in range(bands):
        rows = packed_ref[band * features : (band + 1) * features, :] * weight
        if band == 0:
            rows = rows + diag_terms
        for i in range(regions):
            j = (i + band) % regions
            cols_ref[min(i, j), max(i, j) : max(i, j) + 1, :] = rows[i : i + 1]
    cross = packed_ref[bands * features : (bands + 1) * features, :] * weight
    for i in range(regions):
        cols_ref[i, regions : regions + 1, :] = cross[i : i + 1]
    cols_ref[regions, regions : regions + 1, :] = cross[regions:] + diag_terms[regions:]
    gradient = packed_ref[(bands + 1) * features : (bands + 2) * features, :] * weight
    gradient = gradient + ridge_weight * policy + barrier_weight * 2.0 * policy / margin_sq
    grad_sq = jnp.sum(gradient * gradient, axis=0, keepdims=True)

    positions = lax.broadcasted_iota(jnp.int32, gradient.shape, 0)
    inverses, forward = [], []
    running = gradient
    forward_sq = jnp.zeros_like(weight)
    for k in range(features):
        column = cols_ref[k]
        inverse = 1.0 / jnp.sqrt(column[k : k + 1])
        column = jnp.where(positions >= k, column * inverse, 0.0)
        cols_ref[k] = column
        value = running[k : k + 1] * inverse
        running = running - column * value
        forward_sq = forward_sq + value * value
        inverses.append(inverse)
        forward.append(value)
        for j in range(k + 1, features):
            base = j // 8 * 8
            cols_ref[j, base:, :] = cols_ref[j, base:, :] - column[base:] * column[j : j + 1]
    solved = jnp.zeros_like(gradient)
    for k in reversed(range(features)):
        value = (
            forward[k] - jnp.sum(cols_ref[k] * solved, axis=0, keepdims=True)
        ) * inverses[k]
        solved = jnp.where(positions == k, value, solved)
    out_ref[...] = jnp.zeros_like(out_ref)
    out_ref[:features, :] = -solved
    out_ref[features : features + 1, :] = forward_sq
    out_ref[features + 1 : features + 2, :] = grad_sq


def greet(partners):
    barrier = pltpu.get_barrier_semaphore()
    for partner in partners:
        pl.semaphore_signal(
            barrier, inc=1, device_id=partner, device_id_type=pl.DeviceIdType.MESH
        )
    pl.semaphore_wait(barrier, len(partners))


def share_steps(samples, ring, features, meanwhile, solved_ref, all_ref, sums_ref, got_ref, mine_ref, far_ref, sends, recvs):
    me, place = lax.axis_index("sample"), lax.axis_index("line")
    peers = [lax.rem(me + i, samples) for i in range(1, samples)]
    lines = [lax.rem(place + i, ring) for i in range(1, ring)]
    copies = []
    for slot, peer in enumerate(peers):
        copies.append(
            pltpu.make_async_remote_copy(
                src_ref=solved_ref,
                dst_ref=got_ref.at[slot],
                send_sem=sends.at[slot],
                recv_sem=recvs.at[slot],
                device_id={"sample": peer},
                device_id_type=pl.DeviceIdType.MESH,
            )
        )
        copies[-1].start()
    total = solved_ref[features:, :]
    for slot in range(samples - 1):
        copies[slot].wait_recv()
        total = total + got_ref[slot, features:, :]
    mine_ref[...] = total
    all_ref[me] = solved_ref[:features, :]
    for slot in range(samples - 1):
        source = lax.rem(me + samples - 1 - slot, samples)
        all_ref[source] = got_ref[slot, :features, :]
    far = []
    for slot, line in enumerate(lines):
        far.append(
            pltpu.make_async_remote_copy(
                src_ref=mine_ref,
                dst_ref=far_ref.at[slot],
                send_sem=sends.at[samples - 1 + slot],
                recv_sem=recvs.at[samples - 1 + slot],
                device_id={"line": line},
                device_id_type=pl.DeviceIdType.MESH,
            )
        )
        far[-1].start()
    meanwhile()
    total = mine_ref[...]
    for slot in range(ring - 1):
        far[slot].wait_recv()
        total = total + far_ref[slot]
    sums_ref[...] = total
    for copy in copies + far:
        copy.wait_send()


def split(value):
    top = value.astype(jnp.bfloat16)
    return top, (value - top.astype(jnp.float32)).astype(jnp.bfloat16)


def dot3(left, right):
    left_top, left_rest = split(left)
    right_top, right_rest = split(right)

    def product(a, b):
        return lax.dot_general(a, b, (((1,), (0,)), ((), ())), preferred_element_type=jnp.float32)

    return product(left_top, right_top) + (
        product(left_top, right_rest) + product(left_rest, right_top)
    )


def split_rows(width, total, ring):
    rows = (width + 15 + 15) // 16 * 16
    starts = [min(piece * width // 16 * 16, total - rows) for piece in range(ring)]
    return rows, starts


def newton_kernel(
    samples, ring, chunk, block, group,
    wind_ref, ptdf_ref, weights_hbm, ends_hbm, ratings_hbm, monitored_hbm, base_hbm, cost_hbm,
    policy_hbm,
    policy_out, flow_out, decrement_out, norm_out,
    diff_ref, factors_ref, all_ref, sums_ref, winds, grids, region_mix, stage, table, found, spread, outbox, inbox, mix_inbox,
    packed, weight_mine, policy_mine, cols, solved, step_inbox, mine, far,
    own_sem, stage_sems, send_up, recv_up, send_down, recv_down,
    send_out, recv_out, send_mix, recv_mix, send_rest, recv_rest, send_step, recv_step,
    rest_out, rest_in, weights_ref, ends_ref, ratings_ref, monitored_ref, base_ref, cost_ref,
    policy_ref, small_sems,
):
    me, mine_s = lax.axis_index("line"), lax.axis_index("sample")
    regions = weights_hbm.shape[0]
    features = regions + 1
    width, scen_here = wind_ref.shape
    total, lines_here = ptdf_ref.shape
    grid_lines = ends_hbm.shape[1]
    share = lines_here // samples
    chunks = scen_here // chunk
    blocks = lines_here // block
    bands = (regions + 1) // 2
    reach = ring - 1
    f32, bf16 = jnp.float32, jnp.bfloat16
    peers = [lax.rem(mine_s + i, samples) for i in range(1, samples)]
    greet(
        [{"line": lax.rem(me + i, ring)} for i in range(1, ring)]
        + [{"sample": peer} for peer in peers]
    )

    def rows_of(step):
        return pl.ds(pl.multiple_of(step * chunk, chunk), chunk)

    middle = max(width // 2 // 16 * 16, 16)
    halves = ((0, middle), (middle, width - middle))
    ahead = 3

    def slot_of(step, hops, half):
        return (step * reach + hops - 1) * 2 + half

    def transfer(step, hops, side, half):
        piece = me - side * (hops - 1)
        slot = slot_of(step, hops, half)
        rows = rows_of(step)
        depth = pl.ds(*halves[half])
        first = isinstance(hops, int) and hops == 1
        source = wind_ref.at[depth, rows] if first else winds.at[piece, depth, rows]
        sends_, recvs = (send_up, recv_up) if side == 1 else (send_down, recv_down)
        return pltpu.make_async_remote_copy(
            src_ref=source,
            dst_ref=winds.at[piece, depth, rows],
            send_sem=sends_.at[slot],
            recv_sem=recvs.at[slot],
            device_id={"line": me + side},
            device_id_type=pl.DeviceIdType.MESH,
        )

    def sends(hops, side):
        if side == 1:
            return jnp.logical_and(me >= hops - 1, me < ring - 1)
        return jnp.logical_and(me <= ring - hops, me > 0)

    def receives(hops, side):
        return me >= hops if side == 1 else me < ring - hops

    def launch(step, hops, half):
        for side in (1, -1):
            @pl.when(sends(hops, side))
            def _():
                transfer(step, hops, side, half).start()

    def arrival(step, hops, side, half):
        slot = slot_of(step, hops, half)
        here = winds.at[me - side * hops, pl.ds(*halves[half]), rows_of(step)]
        pltpu.make_async_remote_copy(
            src_ref=here,
            dst_ref=here,
            send_sem=(send_up if side == 1 else send_down).at[slot],
            recv_sem=(recv_up if side == 1 else recv_down).at[slot],
            device_id={"line": me - side},
            device_id_type=pl.DeviceIdType.MESH,
        ).wait_recv()

    for step in range(min(chunks, ahead)):
        for half in (0, 1):
            launch(step, 1, half)
    own = pltpu.make_async_copy(wind_ref, winds.at[me], own_sem)
    own.start()

    small = [
        pltpu.make_async_copy(source, target, small_sems.at[index])
        for index, (source, target) in enumerate(
            [
                (weights_hbm, weights_ref),
                (ends_hbm, ends_ref),
                (ratings_hbm, ratings_ref),
                (monitored_hbm, monitored_ref),
                (base_hbm, base_ref),
                (cost_hbm, cost_ref),
                (policy_hbm, policy_ref),
            ]
        )
    ]
    for copy in small:
        copy.start()
    stage_rows, starts = split_rows(width, total, ring)

    def staged(piece, index):
        slot = lax.rem(index, 2)
        return pltpu.make_async_copy(
            ptdf_ref.at[
                pl.ds(starts[piece], stage_rows), pl.ds(pl.multiple_of(index * block, block), block)
            ],
            stage.at[slot],
            stage_sems.at[slot],
        )

    region_mix[...] = jnp.zeros_like(region_mix)
    for copy in small:
        copy.wait()
    for piece in range(ring):
        region_mix[piece, :regions, :] = weights_ref[:, width * piece : width * (piece + 1)]
        skip = width * piece - starts[piece]
        staged(piece, 0).start()

        def place(index, carry):
            @pl.when(index + 1 < blocks)
            def _():
                staged(piece, index + 1).start()

            staged(piece, index).wait()
            lines = pl.ds(pl.multiple_of(index * block, block), block)
            grids[piece, :, lines] = stage[lax.rem(index, 2), skip : skip + width, :]
            return carry

        lax.fori_loop(0, blocks, place, 0)

    ends = ends_ref[...]
    rating_all = ratings_ref[...].reshape(1, grid_lines)
    first = rating_all.astype(bf16).astype(f32)
    second = (rating_all - first).astype(bf16).astype(f32)
    third = rating_all - first - second
    table[...] = jnp.zeros_like(table)
    table[:, :grid_lines] = jnp.concatenate(
        [
            (ends // 256).astype(f32),
            lax.rem(ends, 256).astype(f32),
            first,
            second,
            third,
            jnp.zeros_like(first),
        ],
        axis=0,
    ).astype(bf16)
    found[...] = jnp.zeros_like(found)

    def lookup(index, carry):
        where = pl.ds(pl.multiple_of(index * group, group), group)
        hot = (
            lax.broadcasted_iota(jnp.int32, (group, lines_here), 0) + index * group
            == monitored_ref[...]
        )
        found[...] += lax.dot_general(
            table[:, where],
            jnp.where(hot, 1.0, 0.0).astype(bf16),
            (((1,), (0,)), ((), ())),
            preferred_element_type=f32,
        )
        return carry

    lax.fori_loop(0, table.shape[1] // group, lookup, 0)
    from_bus = found[0:1, :] * 256.0 + found[2:3, :]
    to_bus = found[1:2, :] * 256.0 + found[3:4, :]
    rating_row = found[4:5, :] + found[5:6, :] + found[6:7, :]
    found[0:1, :] = from_bus
    found[1:2, :] = to_bus
    for d in range(samples):
        cut = slice(d * share, (d + 1) * share)
        spread[d, :features, :] = policy_ref[:, cut]
        spread[d, features : features + 1, :] = cost_ref[:, cut]
        spread[d, features + 1 : features + 2, :] = rating_row[:, cut]
    policy_mine[...] = spread[mine_s, :features, :]
    weight_mine[...] = spread[mine_s, features : features + 1, :] / (scen_here * samples)
    packed[...] = jnp.zeros_like(packed)
    own.wait()

    forward = (((1,), (0,)), ((), ()))

    def add_piece(step, piece, half):
        rows = rows_of(step)
        low, deep = halves[half]
        depth = pl.ds(low, deep)
        wind = winds[piece, depth, rows]
        turned = wind.T
        groups = [(cut, min(256, deep - cut)) for cut in range(0, deep, 256)]
        yes, no = bf16(1), bf16(0)

        def one(index, carry):
            lines = pl.ds(pl.multiple_of(index * block, block), block)
            local = found[0:2, lines] - (piece * width + low).astype(f32)
            picks = []
            for cut, size in groups:
                inside = local - float(cut)
                inside = jnp.where((inside >= 0) & (inside < size), inside, -1.0).astype(bf16)
                here = lax.broadcasted_iota(jnp.int32, (size, block), 0).astype(f32).astype(bf16)
                picks.append(
                    jnp.where(here == inside[1:2], yes, no)
                    - jnp.where(here == inside[0:1], yes, no)
                )
            flow_out[rows, lines] += lax.dot_general(
                turned, grids[piece, depth, lines], forward, preferred_element_type=f32
            )
            diff_ref[rows, lines] += lax.dot_general(
                turned, jnp.concatenate(picks, axis=0), forward, preferred_element_type=f32
            )
            return carry

        lax.fori_loop(0, blocks, one, 0)
        factors_ref[:, rows] += lax.dot_general(
            region_mix[piece, :, depth], wind, forward, preferred_element_type=f32
        )

    def parcel(step, slot, peer, source):
        spot = step * (samples - 1) + slot
        common = dict(device_id={"sample": peer}, device_id_type=pl.DeviceIdType.MESH)
        return (
            pltpu.make_async_remote_copy(
                src_ref=outbox.at[peer, step],
                dst_ref=inbox.at[source, step],
                send_sem=send_out.at[spot],
                recv_sem=recv_out.at[spot],
                **common,
            ),
            pltpu.make_async_remote_copy(
                src_ref=mix_inbox.at[mine_s, step],
                dst_ref=mix_inbox.at[source, step],
                send_sem=send_mix.at[spot],
                recv_sem=recv_mix.at[spot],
                **common,
            ),
        )

    def remainder(step, slot, peer, source):
        spot = step * (samples - 1) + slot
        return pltpu.make_async_remote_copy(
            src_ref=rest_out.at[peer, step],
            dst_ref=rest_in.at[source, step],
            send_sem=send_rest.at[spot],
            recv_sem=recv_rest.at[spot],
            device_id={"sample": peer},
            device_id_type=pl.DeviceIdType.MESH,
        )

    owners = block // share

    def finish(step):
        rows = rows_of(step)
        turned = factors_ref[:, rows].T
        mix_inbox[mine_s, step] = factors_ref[:, rows]
        for slot, peer in enumerate(peers):
            parcel(step, slot, peer, mine_s)[1].start()

        def one(turn, carry):
            index = lax.rem(mine_s // owners + 1 + turn, blocks)
            lines = pl.ds(pl.multiple_of(index * block, block), block)
            diff = diff_ref[rows, lines]
            flow = (
                flow_out[rows, lines]
                + base_ref[:, lines]
                + dot3(turned, policy_ref[:, lines])
                + policy_ref[regions:, lines] * diff
            )
            flow_out[rows, lines] = flow
            for inner in range(owners):
                cut = slice(inner * share, (inner + 1) * share)
                peer = index * owners + inner
                slot = lax.rem(peer - mine_s - 1 + samples, samples)
                coarse = flow[:, cut].astype(bf16)
                outbox[peer, step, 0] = coarse
                outbox[peer, step, 1] = diff[:, cut].astype(bf16)
                if chunks > 1:
                    @pl.when(step < chunks - 1)
                    def _():
                        rest_out[peer, step] = (flow[:, cut] - coarse.astype(f32)).astype(bf16)

                @pl.when(peer != mine_s)
                def _():
                    parcel(step, slot, peer, mine_s)[0].start()

                    @pl.when(step < chunks - 1)
                    def _():
                        remainder(step, slot, peer, mine_s).start()

            return carry

        lax.fori_loop(0, blocks, one, 0)

    def collect(step, last):
        inbox[mine_s, step] = outbox[mine_s, step]
        if not last:
            rest_in[mine_s, step] = rest_out[mine_s, step]
        rating = spread[mine_s, features + 1 : features + 2, :]

        batch = 2 if samples % 2 == 0 else 1

        def one(turn, carry):
            flows, diffs, mixes = [], [], []
            for inner in range(batch):
                order = turn * batch + inner
                source = lax.rem(mine_s + samples - order, samples)

                @pl.when(order > 0)
                def _():
                    for copy in parcel(step, order - 1, source, source):
                        copy.wait_recv()
                    if not last:
                        remainder(step, order - 1, source, source).wait_recv()

                flow = inbox[source, step, 0].astype(f32)
                if not last:
                    flow = flow + rest_in[source, step].astype(f32)
                flows.append(flow)
                diffs.append(inbox[source, step, 1].astype(f32))
                mixes.append(mix_inbox[source, step])
            flow = jnp.concatenate(flows, axis=0)
            diff = jnp.concatenate(diffs, axis=0)
            factors = jnp.concatenate(mixes, axis=1)
            doubled = jnp.concatenate(
                [factors[:regions], factors[:regions], factors[regions:]], axis=0
            )
            pairs = jnp.concatenate(
                [doubled[d : d + features] * factors for d in range(bands)], axis=0
            )
            prob_up = jax.nn.sigmoid((flow - rating) / smoothing)
            prob_down = jax.nn.sigmoid((-flow - rating) / smoothing)
            slope = prob_up - prob_down
            curve = (prob_up * (1.0 - prob_up) + prob_down * (1.0 - prob_down)) / smoothing
            weighted = curve * diff
            top = bands * features
            low = top + features
            packed[:top, :] += dot3(pairs, curve)
            packed[top : top + regions, :] += dot3(factors, weighted)[:regions]
            packed[top + regions : low, :] += jnp.sum(weighted * diff, axis=0, keepdims=True)
            packed[low : low + regions, :] += dot3(factors, slope)[:regions]
            packed[low + regions : low + features, :] += jnp.sum(
                slope * diff, axis=0, keepdims=True
            )
            return carry

        lax.fori_loop(0, samples // batch, one, 0)

    flow_out[...] = jnp.zeros_like(flow_out)
    diff_ref[...] = jnp.zeros_like(diff_ref)
    factors_ref[...] = jnp.zeros_like(factors_ref)

    def advance(tick, carry):
        @pl.when(tick + ahead < chunks)
        def _():
            for half in (0, 1):
                launch(tick + ahead, 1, half)

        def visit(turn, inner):
            hops = (turn + 1) // 2
            step = tick - jnp.maximum(hops - 1, 0)
            opening = lax.rem(turn, 2) == 1
            piece = me + hops * (1 - 2 * lax.rem(turn, 2))

            @pl.when(jnp.logical_and(step >= 0, step < chunks))
            def _():
                for half in (0, 1):
                    @pl.when(opening)
                    def _():
                        for side in (1, -1):
                            @pl.when(receives(hops, side))
                            def _():
                                arrival(step, hops, side, half)

                        @pl.when(hops < reach)
                        def _():
                            launch(step, hops + 1, half)

                    @pl.when(jnp.logical_and(piece >= 0, piece < ring))
                    def _():
                        add_piece(step, piece, half)

            return inner

        lax.fori_loop(0, 2 * ring - 1, visit, 0)
        done = tick - (reach - 1)

        @pl.when(done >= 0)
        def _():
            finish(done)

        @pl.when(done > 0)
        def _():
            collect(done - 1, False)

        return carry

    lax.fori_loop(0, chunks + reach - 1, advance, 0)
    collect(chunks - 1, True)
    solve_lines(regions, packed, weight_mine, policy_mine, solved, cols)
    def full_step():
        return jnp.concatenate([all_ref[d] for d in range(samples)], axis=1)

    def shifts():
        steps = full_step()

        def one(step, carry):
            rows = rows_of(step)
            turned = factors_ref[:, rows].T
            diff_ref[rows, :] = dot3(turned, steps) + steps[regions:, :] * diff_ref[rows, :]
            return carry

        lax.fori_loop(0, chunks, one, 0)

    share_steps(
        samples, ring, features, shifts, solved, all_ref, sums_ref, step_inbox, mine, far,
        send_step, recv_step,
    )
    sizes = jnp.sqrt(jnp.sum(sums_ref[...], axis=1, keepdims=True))
    decrement_out[...] = sizes[:1]
    norm_out[...] = sizes[1:2]
    scale = 1.0 / (
        1.0 + sizes[:1] / ((barrier_weight * features * lines_here * ring) ** 0.5)
    )
    policy_out[...] = policy_ref[...] + scale * full_step()
    flow_out[...] += scale * diff_ref[...]

    def drain(step, carry):
        def line_drain(hops, inner):
            for side in (1, -1):
                @pl.when(sends(hops, side))
                def _():
                    for half in (0, 1):
                        transfer(step, hops, side, half).wait_send()
            return inner

        for side in (1, -1):
            @pl.when(sends(1, side))
            def _():
                for half in (0, 1):
                    transfer(step, 1, side, half).wait_send()

        lax.fori_loop(2, ring, line_drain, 0)
        for slot, peer in enumerate(peers):
            for copy in parcel(step, slot, peer, mine_s):
                copy.wait_send()

        @pl.when(step < chunks - 1)
        def _():
            for slot, peer in enumerate(peers):
                remainder(step, slot, peer, mine_s).wait_send()

        return carry

    lax.fori_loop(0, chunks, drain, 0)


def newton_steps(
    wind_dev, ptdf, region_weights, incidence, monitored, ratings, base_flow, line_cost, policy
):
    samples, ring = lax.axis_size("sample"), lax.axis_size("line")
    scen_here, width = wind_dev.shape
    lines_here, total = ptdf.shape
    features = policy.shape[0]
    share = lines_here // samples
    chunk = 128
    chunks = scen_here // chunk
    block = 256
    while lines_here % block:
        block //= 2
    group = 512
    table_cols = (incidence.shape[0] + group - 1) // group * group
    stage_rows, _ = split_rows(width, total, ring)
    packed_rows = (features // 2 + 2) * features
    hops = 2 * chunks * (ring - 1)
    parcels = chunks * (samples - 1)
    copies = samples + ring - 2
    vmem = pl.BlockSpec(memory_space=pltpu.VMEM)
    far_off = pl.BlockSpec(memory_space=pltpu.HBM)
    f32, bf16 = jnp.float32, jnp.bfloat16
    dma = pltpu.SemaphoreType.DMA
    return pl.pallas_call(
        lambda *refs: newton_kernel(samples, ring, chunk, block, group, *refs),
        out_shape=(
            pltpu.VMEM((features, lines_here), f32),
            pltpu.VMEM((scen_here, lines_here), f32),
            pltpu.VMEM((1, 1), f32),
            pltpu.VMEM((1, 1), f32),
        ),
        in_specs=[far_off] * 9,
        out_specs=(vmem,) * 4,
        scratch_shapes=[
            pltpu.VMEM((scen_here, lines_here), f32),
            pltpu.VMEM((features, scen_here), f32),
            pltpu.VMEM((samples, features, share), f32),
            pltpu.VMEM((8, share), f32),
            pltpu.VMEM((ring, width, scen_here), bf16),
            pltpu.VMEM((ring, width, lines_here), bf16),
            pltpu.VMEM((ring, features, width), bf16),
            pltpu.VMEM((2, stage_rows, block), bf16),
            pltpu.VMEM((8, table_cols), bf16),
            pltpu.VMEM((8, lines_here), f32),
            pltpu.VMEM((samples, features + 8, share), f32),
            pltpu.VMEM((samples, chunks, 2, chunk, share), bf16),
            pltpu.VMEM((samples, chunks, 2, chunk, share), bf16),
            pltpu.VMEM((samples, chunks, features, chunk), f32),
            pltpu.VMEM((packed_rows, share), f32),
            pltpu.VMEM((1, share), f32),
            pltpu.VMEM((features, share), f32),
            pltpu.VMEM((features, features, share), f32),
            pltpu.VMEM((features + 8, share), f32),
            pltpu.VMEM((samples - 1, features + 8, share), f32),
            pltpu.VMEM((8, share), f32),
            pltpu.VMEM((ring - 1, 8, share), f32),
            dma,
            dma((2,)),
            dma((hops,)),
            dma((hops,)),
            dma((hops,)),
            dma((hops,)),
            dma((parcels,)),
            dma((parcels,)),
            dma((parcels,)),
            dma((parcels,)),
            dma((parcels,)),
            dma((parcels,)),
            dma((copies,)),
            dma((copies,)),
            pltpu.VMEM((samples, chunks, chunk, share), bf16),
            pltpu.VMEM((samples, chunks, chunk, share), bf16),
            pltpu.VMEM(region_weights.shape, bf16),
            pltpu.VMEM(incidence.shape[::-1], jnp.int32),
            pltpu.VMEM(ratings.shape, f32),
            pltpu.VMEM((1, lines_here), jnp.int32),
            pltpu.VMEM((1, lines_here), f32),
            pltpu.VMEM((1, lines_here), f32),
            pltpu.VMEM(policy.shape, f32),
            dma((7,)),
        ],
        compiler_params=pltpu.CompilerParams(
            collective_id=0, has_side_effects=True, vmem_limit_bytes=60000000
        ),
        name="newton_steps",
    )(
        wind_dev.T, ptdf.T, region_weights, incidence.T, ratings, monitored[None, :],
        base_flow[None, :], line_cost[None, :], policy,
    )


def shards(*arrays):
    new_policy, new_flows, decrement, grad_norm = newton_steps(*arrays)
    return new_policy, new_flows, decrement.reshape(()), grad_norm.reshape(())


def solution(mesh):
    placed = (
        P("sample", "line"),
        P("line", None),
        P(),
        P(),
        P("line"),
        P(),
        P("line"),
        P("line"),
        P(None, "line"),
    )
    return jax.shard_map(
        shards,
        mesh=mesh,
        in_specs=placed,
        out_specs=(P(None, "line"), P("sample", "line"), P(), P()),
        check_vma=False,
    )
```
